256 devices in a mesh: gx: 16 (over y, z_hi), gy: 16 (over z_lo, x, core).
Axes of the slice: x: 4, y: 4, z: 8 (z_hi: 4, z_lo: 2; z = z_hi * 2 + z_lo), core: 2. Of those that a mesh axis runs over, the one named last changes fastest.
Arguments:
- liquid_starting_warmth: float32 [64, 256, 1024], P('gx', 'gy'), may hold values from -6 to 6
- liquid_spreading_ratios: float32 [64, 256, 1024], P('gx', 'gy'), may hold values from 0.02 to 0.12
- liquid_advective_ratios: float32 [3, 64, 256, 1024], P(None, 'gx', 'gy'), may hold values from -0.08 to 0.08
- liquid_refresh_flags: int32 [64, 256, 8], P('gx', 'gy'), may hold values 0 or 1
- wall_starting_warmth: float32 [64, 256, 1024], P('gx', 'gy'), may hold values from -6 to 6
- wall_thermal_capacity: float32 [64, 256, 1024], P('gx', 'gy'), may hold values from 0.5 to 2
- thermal_conductance: float32 [64, 256, 1024], P('gx', 'gy'), may hold values from 0.5 to 15
- wall_energy_output: float32 [64, 256, 1024], P('gx', 'gy'), may hold values from -36 to 36
- coupling_partner_lookup: int32 [64, 256], P('gx', 'gy'), may hold values from 0 to 255, each once within a row
Outputs:
- fluid_after: float32 [64, 256, 1024], P('gx', 'gy')
- solid_after: float32 [64, 256, 1024], P('gx', 'gy')
The draws below stay inside these ranges and needn't reach their ends.
Inputs may be any that keep to these rules, and one draw needn't show every extreme that they name: For each first index, the row of coupling_partner_lookup holds every number of 0 to 255 once.
All inputs are finite; a program needn't handle non-finite values. No bound on the sum of `liquid_refresh_flags` on one device may be relied on, other than what follows from the above.
Results may differ from the reference program's by a relative error of at most 0.00023.
Values sent between devices are 32-bit elements; how exact they have to be, the bound alone decides.
A program may use at most 64 MiB of HBM per device.

```python
import math
import jax
import jax.numpy as jnp

VOLUMES_ALONG_Z = 1024
SUBSTEPS = 4
ITERS = 4
ZB = 128
VOLUMES_ALONG_X = 64
VOLUMES_ALONG_Y = 256


def draw_thermal_conductance(key, part):
    baseline = jnp.exp(jax.random.uniform(key, (VOLUMES_ALONG_X, VOLUMES_ALONG_Y, VOLUMES_ALONG_Z), jnp.float32, math.log(0.5), math.log(5.0)))
    ramp_up = 1.0 + 2.0 * jnp.arange(VOLUMES_ALONG_X, dtype=jnp.float32) / (VOLUMES_ALONG_X - 1)
    return baseline * ramp_up[:, None, None]


def draw_wall_energy_output(key, part):
    along_x = 1.0 + 2.0 * jnp.arange(VOLUMES_ALONG_X, dtype=jnp.float32) / (VOLUMES_ALONG_X - 1)
    along_y = 1.0 + 2.0 * jnp.arange(VOLUMES_ALONG_Y, dtype=jnp.float32) / (VOLUMES_ALONG_Y - 1)
    scaling = along_x[:, None, None] * along_y[None, :, None]
    samples = jax.random.truncated_normal(key, -4.0, 4.0, (VOLUMES_ALONG_X, VOLUMES_ALONG_Y, VOLUMES_ALONG_Z), jnp.float32)
    return samples * scaling


def with_ends(entries, rng, least, top_value):
    spot = [jax.random.randint(jax.random.fold_in(rng, axis), (), 0, length) for axis, length in enumerate(entries.shape)]
    widest = entries.shape.index(max(entries.shape))
    beside = spot[:widest] + [(spot[widest] + 1) % entries.shape[widest]] + spot[widest + 1:]
    return entries.at[tuple(spot)].set(least).at[tuple(beside)].set(top_value)


def block_scale(stream_key, dims, cuts, least, largest):
    def one(position, blocks):
        draws = jax.random.uniform(jax.random.fold_in(jax.random.fold_in(stream_key, 6), position), (blocks,), jnp.float32, least / len(cuts), largest / len(cuts))
        return jnp.repeat(jnp.exp(draws), dims[position] // blocks).reshape((-1,) + (1,) * (len(dims) - position - 1))

    gain = one(*cuts[0])
    for cut in cuts[1:]:
        gain = gain * one(*cut)
    return gain


def scatter_about(rng, extent, scale, reach, shards=(), kind=jnp.bfloat16):
    gain = block_scale(rng, extent, shards, -0.22, 0.18) if shards else 1.0
    entries = jax.random.normal(rng, extent, jnp.float32) * scale * gain
    return jnp.minimum(jnp.maximum(entries, -reach), reach).astype(kind)


def setup_inputs(seed: int = 0) -> dict:
    key_list = jax.random.split(jax.random.key(seed), 10)
    return {
        "liquid_starting_warmth": scatter_about(key_list[0], (VOLUMES_ALONG_X, VOLUMES_ALONG_Y, VOLUMES_ALONG_Z), 1.0, 6.0, ((0, 16), (1, 16)), jnp.float32),
        "liquid_spreading_ratios": jnp.clip(jnp.exp(math.log(0.12) - 1.7917595 * jax.random.uniform(key_list[1], (VOLUMES_ALONG_X, VOLUMES_ALONG_Y, VOLUMES_ALONG_Z), jnp.float32) ** block_scale(key_list[1], (VOLUMES_ALONG_X, VOLUMES_ALONG_Y, VOLUMES_ALONG_Z), ((0, 16), (1, 16)), -0.2, 0.2)), 0.02, 0.12),
        "liquid_advective_ratios": jnp.clip(jax.random.uniform(key_list[2], (3, VOLUMES_ALONG_X, VOLUMES_ALONG_Y, VOLUMES_ALONG_Z), jnp.float32, -0.08, 0.08) * block_scale(key_list[2], (3, VOLUMES_ALONG_X, VOLUMES_ALONG_Y, VOLUMES_ALONG_Z), ((1, 16), (2, 16)), -0.4, 0.0), -0.08, 0.08),
        "liquid_refresh_flags": with_ends((jax.random.randint(key_list[3], (VOLUMES_ALONG_X, VOLUMES_ALONG_Y, VOLUMES_ALONG_Z // ZB), 0, 4) < 3).astype(jnp.int32), jax.random.fold_in(key_list[3], 1), 0, 1),
        "wall_starting_warmth": scatter_about(key_list[4], (VOLUMES_ALONG_X, VOLUMES_ALONG_Y, VOLUMES_ALONG_Z), 1.0, 6.0, ((0, 16), (1, 16)), jnp.float32),
        "wall_thermal_capacity": jnp.clip(jnp.exp(math.log(2.0) - 1.3862944 * jax.random.uniform(key_list[5], (VOLUMES_ALONG_X, VOLUMES_ALONG_Y, VOLUMES_ALONG_Z), jnp.float32) ** block_scale(key_list[5], (VOLUMES_ALONG_X, VOLUMES_ALONG_Y, VOLUMES_ALONG_Z), ((0, 16), (1, 16)), -0.2, 0.2)), 0.5, 2.0),
        "thermal_conductance": draw_thermal_conductance(jax.random.fold_in(key_list[9], 71), 0),
        "wall_energy_output": draw_wall_energy_output(jax.random.fold_in(key_list[9], 71), 0),
        "coupling_partner_lookup": jax.vmap(lambda own: jax.random.permutation(own, VOLUMES_ALONG_Y))(jax.random.split(key_list[8], VOLUMES_ALONG_X)).reshape((VOLUMES_ALONG_X, VOLUMES_ALONG_Y)).astype(jnp.int32),
    }


def advance(current_estimate, padded, ghost_row, diffusion, velocity, active_cells):
    below = jnp.concatenate([ghost_row[:, :, None], current_estimate[:, :, :-1]], axis=2)
    above = jnp.concatenate([current_estimate[:, :, 1:], jnp.zeros_like(current_estimate[:, :, :1])], axis=2)
    couples = ((padded[:-2, 1:-1], padded[2:, 1:-1]), (padded[1:-1, :-2], padded[1:-1, 2:]), (below, above))
    spread = -6.0 * current_estimate
    carried = jnp.zeros_like(current_estimate)
    for component in range(3):
        behind, ahead = couples[component]
        spread = spread + behind + ahead
        flow_speed = velocity[component]
        carried = carried + jnp.maximum(flow_speed, 0.0) * (current_estimate - behind) + jnp.minimum(flow_speed, 0.0) * (ahead - current_estimate)
    return current_estimate + active_cells * (diffusion * spread - carried)


def neighbours(field, padded):
    below = jnp.concatenate([jnp.zeros_like(field[:, :, :1]), field[:, :, :-1]], axis=2)
    above = jnp.concatenate([field[:, :, 1:], jnp.zeros_like(field[:, :, :1])], axis=2)
    return (padded[:-2, 1:-1], padded[2:, 1:-1], padded[1:-1, :-2], padded[1:-1, 2:], below, above)


def thermal_flow_operator(field, padded_field, thermal_conductance, bordered_conductance, capacity):
    accumulated = capacity * field
    for near_value, near_cond in zip(neighbours(field, padded_field), neighbours(thermal_conductance, bordered_conductance)):
        accumulated = accumulated + 0.5 * (thermal_conductance + near_cond) * (field - near_value)
    return accumulated


def diagonal_of(thermal_conductance, bordered_conductance, capacity):
    accumulated = capacity
    for near_cond in neighbours(thermal_conductance, bordered_conductance):
        accumulated = accumulated + 0.5 * (thermal_conductance + near_cond)
    return accumulated


def border_margin(field):
    return jnp.pad(field, ((1, 1), (1, 1), (0, 0)))


def reference(liquid_starting_warmth, liquid_spreading_ratios, liquid_advective_ratios, liquid_refresh_flags, wall_starting_warmth, wall_thermal_capacity, thermal_conductance, wall_energy_output, coupling_partner_lookup):
    active_cells = jnp.repeat(liquid_refresh_flags.astype(jnp.float32), ZB, axis=2)
    topmost_layers = wall_starting_warmth[:, :, -1]
    ghost_row = jnp.take_along_axis(topmost_layers, coupling_partner_lookup, axis=1)
    current_estimate = liquid_starting_warmth
    flux_sum = jnp.zeros_like(ghost_row)
    for substep in range(SUBSTEPS):
        flux_sum = flux_sum + (current_estimate[:, :, 0] - ghost_row)
        current_estimate = advance(current_estimate, border_margin(current_estimate), ghost_row, liquid_spreading_ratios, liquid_advective_ratios, active_cells)
    flux_mean = flux_sum / SUBSTEPS
    row_ids = jnp.arange(VOLUMES_ALONG_X, dtype=jnp.int32)[:, None]
    arrived = jnp.zeros_like(flux_mean).at[row_ids, coupling_partner_lookup].add(flux_mean)
    equation_source_term = wall_thermal_capacity * wall_starting_warmth + wall_energy_output
    equation_source_term = equation_source_term.at[:, :, -1].add(arrived)
    bordered_conductance = border_margin(thermal_conductance)
    diagonal = diagonal_of(thermal_conductance, bordered_conductance, wall_thermal_capacity)
    converged_warmth = wall_starting_warmth
    leftover_error = equation_source_term - thermal_flow_operator(converged_warmth, border_margin(converged_warmth), thermal_conductance, bordered_conductance, wall_thermal_capacity)
    scaled = leftover_error / diagonal
    search_heading = scaled
    inner_rz = jnp.sum(leftover_error * scaled)
    for iteration in range(ITERS):
        image = thermal_flow_operator(search_heading, border_margin(search_heading), thermal_conductance, bordered_conductance, wall_thermal_capacity)
        descent_length = inner_rz / jnp.sum(search_heading * image)
        converged_warmth = converged_warmth + descent_length * search_heading
        leftover_error = leftover_error - descent_length * image
        scaled = leftover_error / diagonal
        inner_next = jnp.sum(leftover_error * scaled)
        search_heading = scaled + (inner_next / inner_rz) * search_heading
        inner_rz = inner_next
    return current_estimate, converged_warmth
```

```python
import functools

import jax
import jax.numpy as jnp
from jax import lax
from jax.experimental import pallas as pl
from jax.experimental.pallas import tpu as pltpu
from jax.sharding import PartitionSpec as P

MESH = pl.DeviceIdType.MESH
SUBSTEPS = 4
LANES = 128
EU, EL, EX, EK, EB, EC, EXCHANGES = 0, 4, 7, 8, 9, 13, 15
MERGE = 2
F32 = jnp.float32


def kernel(nx, ny, u_in, dif_in, vel_in, flag_in, x_in, cap_in, k_in, q_in, look_in, u_out, x_out,
           U, HU, SU, L, HL, SL, X, HX, SX, K, HK, SK, B, HB, SB, C, HC, SC,
           CF, W, D, DI, CD, CAP, Q, VEL, DIF, FLAG, LOOK, LKC, GH, FX, DV3, UO, XO,
           TS, TR, PS, PR, AS, AR,
           in_sem, out_sem, xs, xr, ys, yr, ts, tr, ps, pr, a_s, a_r):
    gx, gy = lax.axis_index("gx"), lax.axis_index("gy")
    nr, nc, nz = u_in.shape
    top = nz - LANES
    halves = PS.shape[0]
    per = LANES // nc

    def spot(mx, my):
        return {"device_id": (mx, my), "device_id_type": MESH}

    own = pl.ds(1, nr)
    loads = {}
    for name, src, dst in (
        ("x", x_in, X.at[own]), ("look", look_in, LOOK), ("u", u_in, U.at[0, own]), ("k", k_in, K.at[own]),
        ("flag", flag_in, FLAG), ("dif", dif_in, DIF), ("vel", vel_in, VEL), ("cap", cap_in, CAP), ("q", q_in, Q),
    ):
        loads[name] = pltpu.make_async_copy(src, dst, in_sem.at[len(loads)])
        loads[name].start()

    barrier = pltpu.get_barrier_semaphore()

    def greet_y(d, _):
        pl.semaphore_signal(barrier, inc=1, **spot(gx, lax.rem(gy + d, ny)))
        return 0

    def greet_x(d, _):
        pl.semaphore_signal(barrier, inc=1, **spot(lax.rem(gx + d, nx), gy))
        return 0

    lax.fori_loop(1, ny, greet_y, 0)
    lax.fori_loop(1, nx, greet_x, 0)

    for at_edge, row, side in ((gx == 0, 0, None), (gx == nx - 1, nr + 1, None), (gy == 0, None, 0), (gy == ny - 1, None, 1)):
        @pl.when(at_edge)
        def _(row=row, side=side):
            if side is None:
                for ext in (U, L, B, C):
                    ext[:, row] = jnp.zeros((ext.shape[0], *ext.shape[2:]), F32)
                for ext in (X, K):
                    ext[row] = jnp.zeros(ext.shape[1:], F32)
            else:
                for rim in (HU, HL, HB, HC, HX, HK):
                    rim[:, side] = jnp.zeros((rim.shape[0], *rim.shape[2:]), F32)

    up_x, dn_x, up_y, dn_y = lax.rem(gx + 1, nx), lax.rem(gx + nx - 1, nx), lax.rem(gy + 1, ny), lax.rem(gy + ny - 1, ny)

    def x_pair(ext, e):
        return (
            pltpu.make_async_remote_copy(ext.at[nr], ext.at[0], xs.at[e, 0], xr.at[e, 0], **spot(up_x, gy)),
            pltpu.make_async_remote_copy(ext.at[1], ext.at[nr + 1], xs.at[e, 1], xr.at[e, 1], **spot(dn_x, gy)),
        )

    def y_pair(stage, rim, e):
        return (
            pltpu.make_async_remote_copy(stage.at[1], rim.at[0], ys.at[e, 0], yr.at[e, 0], **spot(gx, up_y)),
            pltpu.make_async_remote_copy(stage.at[0], rim.at[1], ys.at[e, 1], yr.at[e, 1], **spot(gx, dn_y)),
        )

    def start(pair, g, n):
        @pl.when(g < n - 1)
        def _():
            pair[0].start()

        @pl.when(g > 0)
        def _():
            pair[1].start()

    def arrive(pair, g, n):
        @pl.when(g > 0)
        def _():
            pair[0].wait_recv()

        @pl.when(g < n - 1)
        def _():
            pair[1].wait_recv()

    def leave(pair, g, n):
        @pl.when(g < n - 1)
        def _():
            pair[0].wait_send()

        @pl.when(g > 0)
        def _():
            pair[1].wait_send()

    def arrive_both(ext, stage, rim, e):
        arrive(y_pair(stage, rim, e), gy, ny)
        arrive(x_pair(ext, e), gx, nx)

    def leave_both(ext, stage, rim, e):
        leave(y_pair(stage, rim, e), gy, ny)
        leave(x_pair(ext, e), gx, nx)

    links = {}
    for k in range(4):
        links["u", k] = (U.at[k], SU.at[k], HU.at[k], EU + k)
        links["b", k] = (B.at[k], SB.at[k], HB.at[k], EB + k)
    for k in range(3):
        links["l", k] = (L.at[k], SL.at[k], HL.at[k], EL + k)
    for k in range(2):
        links["c", k] = (C.at[k], SC.at[k], HC.at[k], EC + k)
    links["x", 0] = (X, SX.at[0], HX.at[0], EX)
    links["k", 0] = (K, SK.at[0], HK.at[0], EK)

    def rows(body, first=0, count=None, step=1):
        def one(t, _):
            body(first + t * step)
            return 0

        lax.fori_loop(0, nr if count is None else count, one, 0)

    def put(name, i, value):
        ext, stage, _, _ = links[name]
        ext[i + 1] = value
        stage[0, pl.ds(i, 1)] = value[0:1]
        stage[1, pl.ds(i, 1)] = value[nc - 1:nc]

    def produce(name, value_of):
        ext, stage, rim, e = links[name]
        rows(lambda i: put(name, i, value_of(i)), 0, 2, nr - 1)
        start(x_pair(ext, e), gx, nx)
        rows(lambda i: put(name, i, value_of(i)), 1, nr - 2)
        start(y_pair(stage, rim, e), gy, ny)

    def stage_and_send(name):
        ext, stage, rim, e = links[name]
        start(x_pair(ext, e), gx, nx)

        def body(i):
            stage[0, pl.ds(i, 1)] = ext[i + 1, 0:1]
            stage[1, pl.ds(i, 1)] = ext[i + 1, nc - 1:nc]

        rows(body)
        start(y_pair(stage, rim, e), gy, ny)

    def await_halo(name):
        arrive_both(*links[name])

    def around(name, i, low=None):
        ext, _, rim, _ = links[name]
        c = ext[i + 1]
        width = c.shape[1]
        sub = lax.broadcasted_iota(jnp.int32, c.shape, 0)
        lane = lax.broadcasted_iota(jnp.int32, c.shape, 1)
        zero = jnp.zeros_like(c)
        return c, (
            ext[i],
            ext[i + 2],
            jnp.where(sub == 0, rim[0, pl.ds(i, 1)], pltpu.roll(c, 1, 0)),
            jnp.where(sub == nc - 1, rim[1, pl.ds(i, 1)], pltpu.roll(c, nc - 1, 0)),
            jnp.where(lane == 0, zero if low is None else low, pltpu.roll(c, 1, 1)),
            jnp.where(lane == width - 1, zero, pltpu.roll(c, width - 1, 1)),
        )

    def fluid(name, i):
        c, near = around(name, i, GH[i][:, 0:1])
        width = c.shape[1]
        total = CF[6, i, :, 0:width] * c
        for n in range(6):
            total = total + CF[n, i, :, 0:width] * near[n]
        return total

    def scaled_image(name, i):
        c, near = around(name, i)
        lanes = pl.ds(nz - c.shape[1], c.shape[1])
        total = CD[i, :, lanes] * c
        for n in range(6):
            total = total + W[n, i, :, lanes] * (c - near[n])
        return total

    def fluid_coefficients():
        def body(i):
            flag = FLAG[i].astype(F32)
            on = jnp.concatenate([jnp.broadcast_to(flag[:, b:b + 1], (nc, LANES)) for b in range(nz // LANES)], axis=1)
            dif = DIF[i]
            size = 6.0 * dif
            for d in range(3):
                vel = VEL[d, i]
                CF[2 * d, i] = on * (dif + jnp.maximum(vel, 0.0))
                CF[2 * d + 1, i] = on * (dif - jnp.minimum(vel, 0.0))
                size = size + jnp.abs(vel)
            CF[6, i] = 1.0 - on * size

        rows(body)

    def solid_coefficients():
        def body(i):
            c, near = around(("k", 0), i)
            cap = CAP[i]
            total = cap
            faces = [0.5 * (c + v) for v in near]
            for face in faces:
                total = total + face
            inverse = 1.0 / total
            D[i] = total
            DI[i] = inverse
            CD[i] = cap * inverse
            for n in range(6):
                W[n, i] = faces[n] * inverse

        rows(body)

    def first_scaled(i):
        c, near = around(("x", 0), i)
        total = DI[i] * Q[i]
        for n in range(6):
            total = total - W[n, i] * (c - near[n])
        return total

    def send_all(src_of, slots, me, n, peer_of, ssem, rsem):
        def one(d, _):
            peer = lax.rem(me + d, n)
            pltpu.make_async_remote_copy(src_of(peer), slots.at[me], ssem, rsem, **spot(*peer_of(peer))).start()
            return 0

        lax.fori_loop(1, n, one, 0)

    def all_arrived(slots, n, ssem, rsem, peer_of, me):
        most = slots.at[pl.ds(0, n - 1)]
        done = pltpu.make_async_remote_copy(most, most, ssem, rsem, **spot(*peer_of(lax.rem(me + 1, n))))
        done.wait_recv()
        done.wait_send()

    def in_row(p):
        return gx, p

    def in_column(p):
        return p, gy

    sub = lax.broadcasted_iota(jnp.int32, (nc, LANES), 0)
    lane = lax.broadcasted_iota(jnp.int32, (nc, LANES), 1)
    mine = lane == lax.rem(gy, per) * nc + sub

    loads["x"].wait()
    TS[...] = jnp.zeros_like(TS)
    for i in range(nr):
        TS[i:i + 1] = jnp.sum(jnp.where(mine, X[i + 1, :, nz - 1:nz], 0.0), axis=0, keepdims=True)
    TR[gy] = TS[...]
    loads["u"].wait()

    def low_start(i):
        put(("l", 0), i, U[0, i + 1, :, 0:LANES])

    rows(low_start)
    loads["look"].wait()
    look = LOOK[...].astype(F32)
    for i in range(nr):
        here = jnp.broadcast_to(look[i:i + 1], (nc, nc))
        a = lax.broadcasted_iota(jnp.int32, (nc, nc), 0)
        b = lax.broadcasted_iota(jnp.int32, (nc, nc), 1)
        LKC[i] = jnp.broadcast_to(jnp.sum(jnp.where(a == b, here, 0.0), axis=1, keepdims=True), (nc, LANES)).astype(jnp.int32)

    pl.semaphore_wait(barrier, nx + ny - 2)
    send_all(lambda p: TS, TR, gy, ny, in_row, ts, tr)
    ext, stage, rim, e = links["l", 0]
    start(x_pair(ext, e), gx, nx)
    start(y_pair(stage, rim, e), gy, ny)
    loads["k"].wait()
    stage_and_send(("k", 0))
    for name in ("flag", "dif", "vel"):
        loads[name].wait()
    fluid_coefficients()

    all_arrived(TR, ny, ts, tr, in_row, gy)
    for i in range(nr):
        ghost = jnp.zeros((nc, LANES), F32)
        for h in range(halves):
            line = TR[h * per, i:i + 1]
            for s in range(1, min(per, ny)):
                line = line + TR[h * per + s, i:i + 1]
            ghost = ghost + jnp.where(LKC[i] == lane + h * LANES, line, 0.0)
        GH[i] = jnp.broadcast_to(jnp.sum(ghost, axis=1, keepdims=True), (nc, LANES))

    def flux_start(i):
        FX[i] = L[0, i + 1] - GH[i]

    rows(flux_start)
    await_halo(("l", 0))

    def low_step(k):
        def value(i):
            new = fluid(("l", k), i)
            FX[i] = FX[i] + (new - GH[i])
            return new

        return value

    produce(("l", 1), low_step(0))
    stage_and_send(("x", 0))
    await_halo(("l", 1))
    produce(("l", 2), low_step(1))
    stage_and_send(("u", 0))
    loads["cap"].wait()
    loads["q"].wait()
    await_halo(("k", 0))
    solid_coefficients()
    await_halo(("l", 2))
    rows(low_step(2))

    for h in range(halves):
        PS[h] = jnp.zeros(PS.shape[1:], F32)
    for i in range(nr):
        flux = FX[i][:, 0:1] / SUBSTEPS
        for h in range(halves):
            PS[h, i:i + 1] = jnp.sum(jnp.where(LKC[i] == lane + h * LANES, flux, 0.0), axis=0, keepdims=True)
    PR[gy] = PS[gy // per]
    send_all(lambda p: PS.at[p // per], PR, gy, ny, in_row, ps, pr)

    await_halo(("x", 0))
    produce(("b", 0), first_scaled)

    all_arrived(PR, ny, ps, pr, in_row, gy)
    total = PR[0]
    for s in range(1, ny):
        total = total + PR[s]
    GH_lane = lane == LANES - 1
    for i in range(nr):
        came = jnp.sum(jnp.where(mine, total[i:i + 1], 0.0), axis=1, keepdims=True)
        put(("c", 0), i, jnp.where(GH_lane, DI[i, :, top:nz] * came, 0.0))
    ext, stage, rim, e = links["c", 0]
    start(x_pair(ext, e), gx, nx)
    start(y_pair(stage, rim, e), gy, ny)

    await_halo(("u", 0))
    produce(("u", 1), lambda i: fluid(("u", 0), i))

    await_halo(("b", 0))
    produce(("b", 1), lambda i: scaled_image(("b", 0), i))
    await_halo(("c", 0))
    produce(("c", 1), lambda i: scaled_image(("c", 0), i))

    await_halo(("c", 1))

    def top_third(i):
        C[2, i + 1] = C[1, i + 1] - scaled_image(("c", 1), i)

    rows(top_third)

    def third(i):
        value = B[1, i + 1] - scaled_image(("b", 1), i)
        return jnp.concatenate([value[:, 0:top], value[:, top:nz] + C[2, i + 1]], axis=1)

    await_halo(("b", 1))
    produce(("b", 2), third)

    for k in range(MERGE):
        leave_both(*links["b", k])

    def merge(i):
        for k in range(MERGE):
            B[k, i + 1, :, top:nz] = B[k, i + 1, :, top:nz] + C[k, i + 1]

    rows(merge)

    tiles = nz // LANES

    def sums_of(dst, first, count, body):
        def one(t, acc):
            i, b = t // tiles, lax.rem(t, tiles)
            at = pl.ds(pl.multiple_of(b * LANES, LANES), LANES)
            return tuple(a + v for a, v in zip(acc, body(i, at)))

        acc = lax.fori_loop(0, nr * tiles, one, tuple(jnp.zeros((nc, LANES), F32) for _ in range(count)))
        for r, a in enumerate(acc):
            dst[first + r:first + r + 1] = jnp.sum(a, axis=0, keepdims=True)

    def spread_row(use):
        AR[use, 0, gy] = AS[use, 0]
        send_all(lambda p: AS.at[use, 0], AR.at[use, 0], gy, ny, in_row, a_s.at[use, 0], a_r.at[use, 0])

    def spread_column(use):
        all_arrived(AR.at[use, 0], ny, a_s.at[use, 0], a_r.at[use, 0], in_row, gy)
        line = AR[use, 0, 0]
        for s in range(1, ny):
            line = line + AR[use, 0, s]
        AS[use, 1] = line
        AR[use, 1, gx] = line
        send_all(lambda p: AS.at[use, 1], AR.at[use, 1], gx, nx, in_column, a_s.at[use, 1], a_r.at[use, 1])

    def collected(use):
        all_arrived(AR.at[use, 1], nx, a_s.at[use, 1], a_r.at[use, 1], in_column, gx)
        line = AR[use, 1, 0]
        for s in range(1, nx):
            line = line + AR[use, 1, s]
        return jnp.sum(line, axis=1, keepdims=True)

    def two(i, at):
        b0 = B[0, i + 1, :, at]
        weighted = D[i, :, at] * b0
        return weighted * b0, weighted * B[1, i + 1, :, at]

    AS[0, 0] = jnp.zeros(AS.shape[2:], F32)
    sums_of(AS.at[0, 0], 0, 2, two)
    spread_row(0)

    await_halo(("u", 1))
    produce(("u", 2), lambda i: fluid(("u", 1), i))

    spread_column(0)
    await_halo(("b", 2))
    produce(("b", 3), lambda i: 2.0 * (B[2, i + 1] - scaled_image(("b", 2), i)) - B[1, i + 1])

    pair = collected(0)
    rho = pair[1:2] / pair[0:1]

    def thirteen(i, at):
        c0, c1, c2, c3 = (B[k, i + 1, :, at] for k in range(4))
        m1 = c1 - c2
        m2 = c2 - 0.5 * (c3 + c1)
        v1 = c1 - rho * c0
        v2 = c2 - rho * (c0 - c1)
        v3 = c3 - rho * (c0 - 2.0 * (c1 + c2))
        weight = D[i, :, at]
        w0, w1, w2, w3 = (weight * v for v in (c0, v1, v2, v3))
        DV3[i, :, at] = w3
        n1 = m1 - rho * c1
        n2 = m2 - rho * c2
        n3 = rho * (c1 - 2.0 * (m1 + m2))
        return (
            w0 * c0, w1 * c0, w2 * c0, w3 * c0,
            w0 * c1, w1 * c1, w2 * c1, w3 * c1,
            w1 * n1, w2 * n1, w3 * n1,
            w2 * n2, w3 * n2,
            -(w3 * n3),
        )

    AS[1, 0] = jnp.zeros(AS.shape[2:], F32)
    sums_of(AS.at[1, 0], 0, 14, thirteen)

    await_halo(("u", 2))
    produce(("u", 3), lambda i: fluid(("u", 2), i))

    await_halo(("b", 3))

    def last(i, acc):
        value = DV3[i] * scaled_image(("b", 3), i)
        for b in range(tiles):
            acc = acc + value[:, b * LANES:(b + 1) * LANES]
        return acc

    AS[1, 0, 14:15] = jnp.sum(lax.fori_loop(0, nr, last, jnp.zeros((nc, LANES), F32)), axis=0, keepdims=True)
    spread_row(1)

    await_halo(("u", 3))
    rows(lambda i: UO.__setitem__(i, fluid(("u", 3), i)))
    u_done = pltpu.make_async_copy(UO, u_out, out_sem.at[0])
    u_done.start()

    spread_column(1)
    col = collected(1)
    e = [col[r:r + 1] for r in range(15)]
    g = e[0:4]
    H = {(0, 0): e[4], (1, 0): e[5], (2, 0): e[6], (3, 0): e[7], (1, 1): e[8], (2, 1): e[9], (3, 1): e[10],
         (2, 2): e[11], (3, 2): e[12], (3, 3): e[13] + e[14]}
    inv, low = {}, {}
    for j in range(4):
        pivot = H[j, j]
        for m in range(j):
            pivot = pivot - low[j, m] * H[j, m]
        inv[j] = jnp.where(pivot > 0.0, 1.0 / pivot, 0.0)
        for i in range(j + 1, 4):
            value = H[i, j]
            for m in range(j):
                value = value - low[j, m] * H[i, m]
            H[i, j] = value
            low[i, j] = value * inv[j]
    y = list(g)
    for i in range(4):
        for m in range(i):
            y[i] = y[i] - low[i, m] * y[m]
    y = [y[i] * inv[i] for i in range(4)]
    for i in range(3, -1, -1):
        for m in range(i + 1, 4):
            y[i] = y[i] - low[m, i] * y[m]
    f0 = y[0] - rho * (y[1] + y[2] + y[3])
    f1 = y[1] + rho * (y[2] + 2.0 * y[3])
    f2 = y[2] + 2.0 * rho * y[3]

    def finish(i):
        XO[i] = X[i + 1] + ((f0 * B[0, i + 1] + f1 * B[1, i + 1]) + (f2 * B[2, i + 1] + y[3] * B[3, i + 1]))

    rows(finish)
    x_done = pltpu.make_async_copy(XO, x_out, out_sem.at[1])
    x_done.start()

    for name, link in links.items():
        if name not in (("b", 0), ("b", 1)):
            leave_both(*link)
    u_done.wait()
    x_done.wait()


def solution(mesh):
    nx, ny = mesh.shape["gx"], mesh.shape["gy"]

    def local(u, dif, vel, flag, x, cap, k, q, look):
        nr, nc, nz = u.shape
        halves = max(1, nc * ny // LANES)
        most = max(nx, ny)
        vm = lambda *shape: pltpu.VMEM(shape, F32)
        dma = lambda *shape: pltpu.SemaphoreType.DMA(shape)

        def linked(count, width):
            return [vm(count, nr + 2, nc, width), vm(count, 2, nr, width), vm(count, 2, nr, width)]

        def linked_one(width):
            return [vm(nr + 2, nc, width), vm(1, 2, nr, width), vm(1, 2, nr, width)]

        block = (nr, nc, nz)
        scratch = [
            *linked(4, nz), *linked(3, LANES), *linked_one(nz), *linked_one(nz), *linked(4, nz), *linked(3, LANES),
            vm(7, *block), vm(6, *block), vm(*block), vm(*block), vm(*block), vm(*block), vm(*block),
            vm(3, *block), vm(*block), pltpu.VMEM(flag.shape, jnp.int32), pltpu.VMEM(look.shape, jnp.int32),
            pltpu.VMEM((nr, nc, LANES), jnp.int32), vm(nr, nc, LANES), vm(nr, nc, LANES), vm(*block), vm(*block), vm(*block),
            vm(8, LANES), vm(ny, 8, LANES), vm(halves, 8, LANES), vm(ny, 8, LANES),
            vm(2, 2, 16, LANES), vm(2, 2, most, 16, LANES),
            dma(9), dma(2), dma(EXCHANGES, 2), dma(EXCHANGES, 2), dma(EXCHANGES, 2), dma(EXCHANGES, 2),
            dma(), dma(), dma(), dma(), dma(2, 2), dma(2, 2),
        ]
        any_space = pl.BlockSpec(memory_space=pl.ANY)
        return pl.pallas_call(
            functools.partial(kernel, nx, ny),
            out_shape=(jax.ShapeDtypeStruct(block, F32), jax.ShapeDtypeStruct(block, F32)),
            in_specs=[any_space] * 9,
            out_specs=(any_space, any_space),
            scratch_shapes=scratch,
            compiler_params=pltpu.CompilerParams(collective_id=0, has_side_effects=True, vmem_limit_bytes=40 * 1024 * 1024),
            name="window",
        )(u, dif, vel, flag, x, cap, k, q, look)

    spec = P("gx", "gy", None)
    return jax.shard_map(
        local,
        mesh=mesh,
        in_specs=(spec, spec, P(None, "gx", "gy", None), spec, spec, spec, spec, spec, P("gx", "gy")),
        out_specs=(spec, spec),
        check_vma=False,
    )
```

```python
import functools

import jax
import jax.numpy as jnp
from jax import lax
from jax.experimental import pallas as pl
from jax.experimental.pallas import tpu as pltpu
from jax.sharding import PartitionSpec as P

MESH = pl.DeviceIdType.MESH
SUBSTEPS = 4
LANES = 128
X_U, X_L, X_X, X_K, X_B, X_C, EXCHANGES = 0, 4, 7, 8, 9, 13, 14
ORDER = (
    "T", "L0", "K", "X", "LK", "CF", "G", "L1", "E", "W", "L2", "B0", "L3", "EW", "U0", "B1", "C", "R1", "B2", "U1",
    "R2", "B3", "R3", "U2", "H", "U3", "A2", "U4", "A3",
)
F32 = jnp.float32


def kernel(nx, ny, u_in, dif_in, vel_in, flag_in, x_in, cap_in, k_in, q_in, look_in, u_out, x_out,
           U, HU, SU, L, HL, SL, X, HX, SX, K, HK, SK, B, HB, SB, C, HC, SC,
           CF, W, D, DI, CD, CAP, Q, VEL, DIF, FLAG, LOOK, LKC, GH, FX, DV3,
           EP, EK, EC, WE, CE, TS, TR, PS, PR, AW, AS, AR,
           in_sem, xs, xr, ys, yr, ts, tr, es, er, ps, pr, a_s, a_r):
    gx, gy = lax.axis_index("gx"), lax.axis_index("gy")
    nr, nc, nz = u_in.shape
    top = nz - LANES
    tiles = nz // LANES
    halves = max(1, nc * ny // LANES)
    per = LANES // nc
    waiting, leaving = {}, {}

    def spot(mx, my):
        return {"device_id": (mx, my), "device_id_type": MESH}

    own = pl.ds(1, nr)
    loads = {}
    for name, src, dst in (
        ("x", x_in, X.at[own]), ("look", look_in, LOOK), ("u", u_in, U.at[0, own]), ("k", k_in, K.at[own]),
        ("flag", flag_in, FLAG), ("dif", dif_in, DIF), ("vel", vel_in, VEL), ("cap", cap_in, CAP), ("q", q_in, Q),
    ):
        loads[name] = pltpu.make_async_copy(src, dst, in_sem.at[len(loads)])
        loads[name].start()

    def loaded(*names):
        for name in names:
            if name in loads:
                loads.pop(name).wait()

    EP[...] = jnp.zeros_like(EP)
    barrier = pltpu.get_barrier_semaphore()

    def greet_y(d, _):
        pl.semaphore_signal(barrier, inc=1, **spot(gx, lax.rem(gy + d, ny)))
        return 0

    def greet_x(d, _):
        pl.semaphore_signal(barrier, inc=1, **spot(lax.rem(gx + d, nx), gy))
        return 0

    def greet_beside(mx):
        def one(d, _):
            pl.semaphore_signal(barrier, inc=1, **spot(mx, lax.rem(gy + d, ny)))
            return 0

        lax.fori_loop(1, ny, one, 0)

    lax.fori_loop(1, ny, greet_y, 0)
    lax.fori_loop(1, nx, greet_x, 0)
    beside = ((gx > 0, lax.rem(gx + nx - 1, nx)), (gx < nx - 1, lax.rem(gx + 1, nx)))
    for there, mx in beside:
        @pl.when(there)
        def _(mx=mx):
            greet_beside(mx)

    def all_here():
        rows_beside = jnp.where(gx > 0, 1, 0) + jnp.where(gx < nx - 1, 1, 0)
        pl.semaphore_wait(barrier, nx + ny - 2 + rows_beside * (ny - 1))

    for at_edge, row, side in ((gx == 0, 0, None), (gx == nx - 1, nr + 1, None), (gy == 0, None, 0), (gy == ny - 1, None, 1)):
        @pl.when(at_edge)
        def _(row=row, side=side):
            if side is None:
                for ext in (U, L, B, C):
                    ext[:, row] = jnp.zeros((ext.shape[0], *ext.shape[2:]), F32)
                for ext in (X, K):
                    ext[row] = jnp.zeros(ext.shape[1:], F32)
            else:
                for rim in (HU, HL, HB, HC, HX, HK):
                    rim[:, side] = jnp.zeros((rim.shape[0], *rim.shape[2:]), F32)

    up_x, dn_x, up_y, dn_y = lax.rem(gx + 1, nx), lax.rem(gx + nx - 1, nx), lax.rem(gy + 1, ny), lax.rem(gy + ny - 1, ny)

    def x_pair(ext, e):
        return (
            pltpu.make_async_remote_copy(ext.at[nr], ext.at[0], xs.at[e, 0], xr.at[e, 0], **spot(up_x, gy)),
            pltpu.make_async_remote_copy(ext.at[1], ext.at[nr + 1], xs.at[e, 1], xr.at[e, 1], **spot(dn_x, gy)),
        )

    def y_pair(stage, rim, e):
        return (
            pltpu.make_async_remote_copy(stage.at[1], rim.at[0], ys.at[e, 0], yr.at[e, 0], **spot(gx, up_y)),
            pltpu.make_async_remote_copy(stage.at[0], rim.at[1], ys.at[e, 1], yr.at[e, 1], **spot(gx, dn_y)),
        )

    def start(pair, g, n):
        @pl.when(g < n - 1)
        def _():
            pair[0].start()

        @pl.when(g > 0)
        def _():
            pair[1].start()

    def arrive(pair, g, n):
        @pl.when(g > 0)
        def _():
            pair[0].wait_recv()

        @pl.when(g < n - 1)
        def _():
            pair[1].wait_recv()

    def leave(pair, g, n):
        @pl.when(g < n - 1)
        def _():
            pair[0].wait_send()

        @pl.when(g > 0)
        def _():
            pair[1].wait_send()

    links = {}
    for k in range(4):
        links["u", k] = (U.at[k], SU.at[k], HU.at[k], X_U + k)
        links["b", k] = (B.at[k], SB.at[k], HB.at[k], X_B + k)
    for k in range(3):
        links["l", k] = (L.at[k], SL.at[k], HL.at[k], X_L + k)
    links["c", 3] = (C.at[0], SC.at[0], HC.at[0], X_C)
    links["x", 0] = (X, SX.at[0], HX.at[0], X_X)
    links["k", 0] = (K, SK.at[0], HK.at[0], X_K)

    def send_x(name):
        ext, _, _, e = links[name]
        start(x_pair(ext, e), gx, nx)

    def send_y(name):
        ext, stage, rim, e = links[name]
        start(y_pair(stage, rim, e), gy, ny)

        def came():
            arrive(y_pair(stage, rim, e), gy, ny)
            arrive(x_pair(ext, e), gx, nx)

        def left():
            leave(y_pair(stage, rim, e), gy, ny)
            leave(x_pair(ext, e), gx, nx)

        waiting[name], leaving[name] = came, left

    def await_halo(*names):
        for name in names:
            if name in waiting:
                waiting.pop(name)()

    def rows(body, first=0, count=None, step=1):
        def one(t, _):
            body(first + t * step)
            return 0

        lax.fori_loop(0, nr if count is None else count, one, 0)

    def put(name, i, value):
        ext, stage, _, _ = links[name]
        ext[i + 1] = value
        stage[0, pl.ds(i, 1)] = value[0:1]
        stage[1, pl.ds(i, 1)] = value[nc - 1:nc]

    def produce(name, value_of):
        rows(lambda i: put(name, i, value_of(i)), 0, 2, nr - 1)
        send_x(name)
        rows(lambda i: put(name, i, value_of(i)), 1, nr - 2)
        send_y(name)

    def stage_and_send(name):
        ext, stage, _, _ = links[name]
        send_x(name)

        def body(i):
            stage[0, pl.ds(i, 1)] = ext[i + 1, 0:1]
            stage[1, pl.ds(i, 1)] = ext[i + 1, nc - 1:nc]

        rows(body)
        send_y(name)

    def around(name, i, low=None):
        ext, _, rim, _ = links[name]
        c = ext[i + 1]
        width = c.shape[1]
        sub = lax.broadcasted_iota(jnp.int32, c.shape, 0)
        lane = lax.broadcasted_iota(jnp.int32, c.shape, 1)
        zero = jnp.zeros_like(c)
        return c, (
            ext[i],
            ext[i + 2],
            jnp.where(sub == 0, rim[0, pl.ds(i, 1)], pltpu.roll(c, 1, 0)),
            jnp.where(sub == nc - 1, rim[1, pl.ds(i, 1)], pltpu.roll(c, nc - 1, 0)),
            jnp.where(lane == 0, zero if low is None else low, pltpu.roll(c, 1, 1)),
            jnp.where(lane == width - 1, zero, pltpu.roll(c, width - 1, 1)),
        )

    def fluid(name, i):
        c, near = around(name, i, GH[i][:, 0:1])
        width = c.shape[1]
        total = CF[6, i, :, 0:width] * c
        for n in range(6):
            total = total + CF[n, i, :, 0:width] * near[n]
        return total

    def scaled_image(name, i):
        c, near = around(name, i)
        lanes = pl.ds(nz - c.shape[1], c.shape[1])
        total = CD[i, :, lanes] * c
        for n in range(6):
            total = total + W[n, i, :, lanes] * (c - near[n])
        return total

    def fluid_coefficients():
        square = (nc, nc)
        diagonal = lax.broadcasted_iota(jnp.int32, square, 0) == lax.broadcasted_iota(jnp.int32, square, 1)

        def body(i):
            flag = FLAG[i].astype(F32)
            blocks = []
            for b in range(tiles):
                column = jnp.sum(jnp.where(diagonal, jnp.broadcast_to(flag[b:b + 1], square), 0.0), axis=1, keepdims=True)
                blocks.append(jnp.broadcast_to(column, (nc, LANES)))
            on = jnp.concatenate(blocks, axis=1)
            dif = DIF[i]
            size = 6.0 * dif
            for d in range(3):
                vel = VEL[d, i]
                CF[2 * d, i] = on * (dif + jnp.maximum(vel, 0.0))
                CF[2 * d + 1, i] = on * (dif - jnp.minimum(vel, 0.0))
                size = size + jnp.abs(vel)
            CF[6, i] = 1.0 - on * size

        rows(body)

    def solid_coefficients():
        def body(i):
            c, near = around(("k", 0), i)
            cap = CAP[i]
            total = cap
            faces = [0.5 * (c + v) for v in near]
            for face in faces:
                total = total + face
            inverse = 1.0 / total
            D[i] = total
            DI[i] = inverse
            CD[i] = cap * inverse
            for n in range(6):
                W[n, i] = faces[n] * inverse

        rows(body)

    def first_scaled(i):
        c, near = around(("x", 0), i)
        total = DI[i] * Q[i]
        for n in range(6):
            total = total - W[n, i] * (c - near[n])
        return total

    def in_row(p):
        return gx, p

    def in_column(p):
        return p, gy

    def send_all(name, src_of, slots, me, n, peer_of, ssem, rsem):
        def one(d, _):
            peer = lax.rem(me + d, n)
            pltpu.make_async_remote_copy(src_of(peer), slots.at[me], ssem, rsem, **spot(*peer_of(peer))).start()
            return 0

        lax.fori_loop(1, n, one, 0)
        most = slots.at[pl.ds(0, n - 1)]
        done = pltpu.make_async_remote_copy(most, most, ssem, rsem, **spot(*peer_of(lax.rem(me + 1, n))))
        waiting[name], leaving[name] = done.wait_recv, done.wait_send

    sub = lax.broadcasted_iota(jnp.int32, (nc, LANES), 0)
    lane = lax.broadcasted_iota(jnp.int32, (nc, LANES), 1)
    mine = lane == lax.rem(gy, per) * nc + sub
    equal = lane == sub

    def collect_top():
        loaded("x", "look")
        for i in range(nr):
            TS[i:i + 1] = jnp.sum(jnp.where(mine, X[i + 1, :, nz - 1:nz], 0.0), axis=0, keepdims=True)
        TR[gy] = TS[...]
        all_here()
        send_all("t", lambda p: TS, TR, gy, ny, in_row, ts, tr)

    def low_start():
        loaded("u")
        rows(lambda i: put(("l", 0), i, U[0, i + 1, :, 0:LANES]))
        send_x(("l", 0))
        send_y(("l", 0))

    def partners():
        look = LOOK[...].astype(F32)
        square = (nc, nc)
        diagonal = lax.broadcasted_iota(jnp.int32, square, 0) == lax.broadcasted_iota(jnp.int32, square, 1)
        for i in range(nr):
            here = jnp.broadcast_to(look[i:i + 1], square)
            column = jnp.sum(jnp.where(diagonal, here, 0.0), axis=1, keepdims=True)
            LKC[i] = jnp.broadcast_to(column, (nc, LANES)).astype(jnp.int32)
        goal = jnp.full((nc, LANES), -1.0, F32)
        for i in range(nr):
            goal = jnp.where(lane == i * nc + sub, LKC[i].astype(F32), goal)
        PS[1:2] = jnp.max(goal, axis=0, keepdims=True)

    def ghosts():
        await_halo("t")
        for i in range(nr):
            ghost = jnp.zeros((nc, LANES), F32)
            for h in range(halves):
                line = TR[h * per, i:i + 1]
                for s in range(1, min(per, ny)):
                    line = line + TR[h * per + s, i:i + 1]
                ghost = ghost + jnp.where(LKC[i] == lane + h * LANES, line, 0.0)
            GH[i] = jnp.broadcast_to(jnp.sum(ghost, axis=1, keepdims=True), (nc, LANES))
            FX[i] = L[0, i + 1] - GH[i]

    def low_step(k):
        def value(i):
            new = fluid(("l", k), i)
            FX[i] = FX[i] + (new - GH[i])
            return new

        return value

    wide = (EP.shape[1], LANES)
    pad = (wide[0] - nc) // 2
    wide_sub = lax.broadcasted_iota(jnp.int32, wide, 0)
    wide_lane = lax.broadcasted_iota(jnp.int32, wide, 1)
    keep = LANES // 16

    def flux_home():
        await_halo(("l", 2))
        rows(low_step(2))
        value = jnp.zeros((nc, LANES), F32)
        for i in range(nr):
            value = jnp.where(lane == i * nc + sub, FX[i][:, 0:1] / SUBSTEPS, value)
        PS[0:1] = jnp.sum(value, axis=0, keepdims=True)
        PR[1, gy] = PS[...]
        send_all("p", lambda p: PS, PR.at[1], gy, ny, in_row, ps.at[1], pr.at[1])
        for there, mx, group in ((gx < nx - 1, lax.rem(gx + 1, nx), 0), (gx > 0, lax.rem(gx + nx - 1, nx), 2)):
            @pl.when(there)
            def _(mx=mx, group=group):
                def one(d, _):
                    peer = lax.rem(gy + d, ny)
                    pltpu.make_async_remote_copy(PS, PR.at[group, gy], ps.at[group], pr.at[group], **spot(mx, peer)).start()
                    return 0

                lax.fori_loop(0, ny, one, 0)

        def whole(group):
            return pltpu.make_async_remote_copy(PR.at[group], PR.at[group], ps.at[group], pr.at[group], **spot(up_x, gy))

        def came():
            for there, group in ((gx > 0, 0), (gx < nx - 1, 2)):
                @pl.when(there)
                def _(group=group):
                    whole(group).wait_recv()

        def left():
            for there, group in ((gx < nx - 1, 0), (gx > 0, 2)):
                @pl.when(there)
                def _(group=group):
                    whole(group).wait_send()

        waiting["p2"], leaving["p2"] = came, left

    def edge_copies():
        loaded("k", "cap")
        total = jnp.zeros((nc, LANES), F32)
        for i in range(nr):
            at = i * 2 * keep
            total = jnp.where((lane >= at) & (lane < at + keep), pltpu.roll(K[i + 1, :, top:nz], at + keep, 1), total)
            total = jnp.where((lane >= at + keep) & (lane < at + 2 * keep), pltpu.roll(CAP[i, :, top:nz], (at + 2 * keep) % LANES, 1), total)
        EP[1, pad:pad + nc] = total
        pairs = []
        for dx in (-1, 0, 1):
            for dy in (-1, 0, 1):
                if dx or dy:
                    src = {0: pl.ds(pad, nc), 1: pl.ds(nc, pad), -1: pl.ds(pad, pad)}[dy]
                    dst = {0: pl.ds(pad, nc), 1: pl.ds(0, pad), -1: pl.ds(pad + nc, pad)}[dy]
                    target = (gx + dx >= 0) & (gx + dx < nx) & (gy + dy >= 0) & (gy + dy < ny)
                    source = (gx - dx >= 0) & (gx - dx < nx) & (gy - dy >= 0) & (gy - dy < ny)
                    to = spot(lax.rem(gx + dx + nx, nx), lax.rem(gy + dy + ny, ny))
                    n = len(pairs)
                    pairs.append((target, source, pltpu.make_async_remote_copy(EP.at[1, src], EP.at[1 - dx, dst], es.at[n], er.at[n], **to)))
        for target, _, copy in pairs:
            pl.when(target)(copy.start)

        def came():
            for _, source, copy in pairs:
                pl.when(source)(copy.wait_recv)

        def left():
            for target, _, copy in pairs:
                pl.when(target)(copy.wait_send)

        waiting["e"], leaving["e"] = came, left

    def wide_around(ref, x, count):
        c = ref[x:x + count]
        return c, (ref[x - 1:x - 1 + count], ref[x + 1:x + 1 + count], pltpu.roll(c, 1, 1), pltpu.roll(c, wide[0] - 1, 1),
                   pltpu.roll(c, 1, 2), pltpu.roll(c, LANES - 1, 2))

    def edge_coefficients():
        await_halo("e")
        for x in range(3 * nr):
            at = x % nr * 2 * keep
            packed_row = EP[x // nr]
            EK[x] = jnp.where(wide_lane >= LANES - keep, pltpu.roll(packed_row, LANES - keep - at, 1), 0.0)
            EC[x] = pltpu.roll(packed_row, LANES - 2 * keep - at, 1)

        x, count = 1, 3 * nr - 2
        block = (count, *wide)
        c, near = wide_around(EK, x, count)
        at_row = lax.broadcasted_iota(jnp.int32, block, 0) + (gx * nr - nr + x)
        across = lax.broadcasted_iota(jnp.int32, block, 1) + (gy * nc - pad)
        along = lax.broadcasted_iota(jnp.int32, block, 2)
        inside = (across >= 0) & (across < ny * nc) & (along >= LANES - keep) & (at_row >= 0) & (at_row < nx * nr)
        near = near[:5] + (jnp.where(along == LANES - 1, 0.0, near[5]),)
        faces = [0.5 * (c + v) for v in near]
        cap = EC[x:x + count]
        total = cap
        for face in faces:
            total = total + face
        inverse = jnp.where(inside, 1.0 / jnp.where(inside, total, 1.0), 0.0)
        for n in range(6):
            WE[n, x:x + count] = faces[n] * inverse
        WE[6, x:x + count] = jnp.where(inside, cap, 0.0) * inverse
        WE[7, x:x + count] = inverse

    def flux_arrives():
        await_halo("p", "p2")
        column = (wide_sub + (gy * nc - pad)).astype(F32)
        for group in range(3):
            parts = []
            for first in range(0, ny, 4):
                total = jnp.zeros(wide, F32)
                for s in range(first, min(first + 4, ny)):
                    total = jnp.where(PR[group, s, 1:2] == column, PR[group, s, 0:1], total)
                parts.append(total)
            total = functools.reduce(jnp.add, parts)
            there = {0: gx > 0, 1: gx >= 0, 2: gx < nx - 1}[group]
            for i in range(nr):
                x = group * nr + i
                came = jnp.sum(jnp.where((wide_lane >= i * nc) & (wide_lane < (i + 1) * nc), total, 0.0), axis=1, keepdims=True)
                CE[0, x] = jnp.where((wide_lane == LANES - 1) & there, WE[7, x] * came, 0.0)
        for k in range(1, 4):
            x, count = 1 + k, 3 * nr - 2 - 2 * k
            c, near = wide_around(CE.at[k - 1], x, count)
            total = WE[6, x:x + count] * c
            for n in range(6):
                total = total + WE[n, x:x + count] * (c - near[n])
            if k > 1:
                total = c - total
            if k > 2:
                total = 2.0 * total - CE[k - 2, x:x + count]
            CE[k, x:x + count] = total
        rows(lambda i: put(("c", 3), i, CE[3, nr + i, pad:pad + nc]))
        send_x(("c", 3))
        send_y(("c", 3))

    def field(k):
        def value(i):
            if k == 1:
                return scaled_image(("b", 0), i)
            last = B[k - 1, i + 1] - scaled_image(("b", k - 1), i)
            return last if k == 2 else 2.0 * last - B[k - 2, i + 1]

        await_halo(("b", k - 1))
        produce(("b", k), value)

    def packed(use, count):
        column = jnp.sum(AW[use], axis=1, keepdims=True)
        return jnp.sum(jnp.where(equal, column, 0.0), axis=0, keepdims=True)

    def added(slots, n):
        line = slots[0]
        for s in range(1, n):
            line = line + slots[s]
        return line

    def spread_row(use):
        line = packed(use, 0)
        AS[use, 0] = line
        AR[use, 0, gy] = line
        send_all(("row", use), lambda p: AS.at[use, 0], AR.at[use, 0], gy, ny, in_row, a_s.at[use, 0], a_r.at[use, 0])

    def spread_column(use):
        await_halo(("row", use))
        line = added(AR.at[use, 0], ny)
        AS[use, 1] = line
        AR[use, 1, gx] = line
        send_all(("column", use), lambda p: AS.at[use, 1], AR.at[use, 1], gx, nx, in_column, a_s.at[use, 1], a_r.at[use, 1])

    def collected(use):
        await_halo(("column", use))
        line = added(AR.at[use, 1], nx)
        return jnp.sum(jnp.where(equal, line, 0.0), axis=1, keepdims=True)

    zeros = jnp.zeros((nc, LANES), F32)

    def sums_of(use, first, count, body, acc=None, begin=0, end=None):
        end = tiles if end is None else end

        def one(t, acc):
            i, b = t // (end - begin), begin + lax.rem(t, end - begin)
            at = pl.ds(pl.multiple_of(b * LANES, LANES), LANES)
            return tuple(a + v for a, v in zip(acc, body(i, at)))

        return lax.fori_loop(0, nr * (end - begin), one, (zeros,) * count if acc is None else acc)

    def store_sums(use, first, acc):
        for r, a in enumerate(acc):
            AW[use, first + r:first + r + 1] = jnp.sum(a, axis=0, keepdims=True)

    def scale_sums():
        def two(i, at):
            b0 = B[0, i + 1, :, at]
            weighted = D[i, :, at] * b0
            return weighted * b0, weighted * B[1, i + 1, :, at]

        AW[0] = zeros
        store_sums(0, 0, sums_of(0, 0, 2, two))
        spread_row(0)

    kept = {}

    def most_sums():
        pair = collected(0)
        rho = jnp.where(pair[0:1] > 0.0, pair[1:2] / pair[0:1], 1.0)
        kept["rho"] = rho

        def terms(fields, i, at):
            c0, c1, c2, c3 = fields
            m1 = c1 - c2
            m2 = c2 - 0.5 * (c3 + c1)
            v1 = c1 - rho * c0
            v2 = c2 - rho * (c0 - c1)
            v3 = c3 - rho * (c0 - 2.0 * (c1 + c2))
            weight = D[i, :, at]
            w0, w1, w2, w3 = (weight * v for v in (c0, v1, v2, v3))
            DV3[i, :, at] = w3
            n1 = m1 - rho * c1
            n2 = m2 - rho * c2
            n3 = rho * (c1 - 2.0 * (m1 + m2))
            return (
                w0 * c0, w1 * c0, w2 * c0, w3 * c0,
                w0 * c1, w1 * c1, w2 * c1, w3 * c1,
                w1 * n1, w2 * n1, w3 * n1,
                w2 * n2, w3 * n2,
                -(w3 * n3),
            )

        AW[1] = zeros
        acc = sums_of(1, 0, 14, lambda i, at: terms([B[k, i + 1, :, at] for k in range(4)], i, at), None, 0, tiles - 1)
        acc = sums_of(1, 0, 14, lambda i, at: terms([B[k, i + 1, :, at] + CE[k, nr + i, pad:pad + nc] for k in range(4)], i, at),
                      acc, tiles - 1, tiles)
        store_sums(1, 0, acc)

    def last_sum():
        def last(i, acc):
            value = DV3[i] * scaled_image(("b", 3), i)
            for b in range(tiles):
                acc = acc + value[:, b * LANES:(b + 1) * LANES]
            return acc

        def last_top(i, acc):
            return acc + DV3[i, :, top:nz] * scaled_image(("c", 3), i)

        await_halo(("b", 3))
        acc = lax.fori_loop(0, nr, last, zeros)
        await_halo(("c", 3))
        acc = lax.fori_loop(0, nr, last_top, acc)
        store_sums(1, 14, (acc,))
        spread_row(1)

    def answer():
        rho = kept["rho"]
        col = collected(1)
        e = [col[r:r + 1] for r in range(15)]
        g = e[0:4]
        H = {(0, 0): e[4], (1, 0): e[5], (2, 0): e[6], (3, 0): e[7], (1, 1): e[8], (2, 1): e[9], (3, 1): e[10],
             (2, 2): e[11], (3, 2): e[12], (3, 3): e[13] + e[14]}
        inv, low = {}, {}
        for j in range(4):
            pivot = H[j, j]
            for m in range(j):
                pivot = pivot - low[j, m] * H[j, m]
            inv[j] = jnp.where(pivot > 0.0, 1.0 / pivot, 0.0)
            for i in range(j + 1, 4):
                value = H[i, j]
                for m in range(j):
                    value = value - low[j, m] * H[i, m]
                H[i, j] = value
                low[i, j] = value * inv[j]
        y = list(g)
        for i in range(4):
            for m in range(i):
                y[i] = y[i] - low[i, m] * y[m]
        y = [y[i] * inv[i] for i in range(4)]
        for i in range(3, -1, -1):
            for m in range(i + 1, 4):
                y[i] = y[i] - low[m, i] * y[m]
        f0 = y[0] - rho * (y[1] + y[2] + y[3])
        f1 = y[1] + rho * (y[2] + 2.0 * y[3])
        f2 = y[2] + 2.0 * rho * y[3]

        y[0:3] = [f0, f1, f2]

        def extra(k, i):
            return CE[k, nr + i, pad:pad + nc]

        def finish(i):
            x_out[i] = X[i + 1] + ((y[0] * B[0, i + 1] + y[1] * B[1, i + 1]) + (y[2] * B[2, i + 1] + y[3] * B[3, i + 1]))
            x_out[i, :, top:nz] = x_out[i, :, top:nz] + (
                (y[0] * extra(0, i) + y[1] * extra(1, i)) + (y[2] * extra(2, i) + y[3] * extra(3, i)))

        rows(finish)

    def coefficients():
        loaded("flag", "dif", "vel")
        fluid_coefficients()

    def solid_start():
        loaded("cap", "q")
        await_halo(("k", 0))
        solid_coefficients()

    def send_input(name, key):
        loaded(key)
        stage_and_send(name)

    def fluid_step(k):
        await_halo(("u", k - 1))
        if k < SUBSTEPS:
            produce(("u", k), lambda i: fluid(("u", k - 1), i))
        else:
            rows(lambda i: u_out.__setitem__(i, fluid(("u", k - 1), i)))

    def low(k):
        await_halo(("l", k - 1))
        produce(("l", k), low_step(k - 1))

    def first_field():
        await_halo(("x", 0))
        produce(("b", 0), first_scaled)

    steps = {
        "T": collect_top, "L0": low_start, "LK": partners, "K": lambda: send_input(("k", 0), "k"), "X": lambda: send_input(("x", 0), "x"),
        "U0": lambda: send_input(("u", 0), "u"), "CF": coefficients, "G": ghosts, "L1": lambda: low(1), "L2": lambda: low(2),
        "L3": flux_home, "W": solid_start, "B0": first_field, "E": edge_copies, "EW": edge_coefficients, "C": flux_arrives, "R1": scale_sums, "R2": lambda: spread_column(0),
        "R3": most_sums, "H": last_sum, "A2": lambda: spread_column(1), "A3": answer,
    }
    for k in range(1, 4):
        steps[f"B{k}"] = functools.partial(field, k)
    for k in range(1, SUBSTEPS + 1):
        steps[f"U{k}"] = functools.partial(fluid_step, k)
    for name in ORDER:
        steps[name]()
    for left in leaving.values():
        left()


def solution(mesh):
    nx, ny = mesh.shape["gx"], mesh.shape["gy"]

    def local(u, dif, vel, flag, x, cap, k, q, look):
        nr, nc, nz = u.shape
        most = max(nx, ny)
        vm = lambda *shape: pltpu.VMEM(shape, F32)
        dma = lambda *shape: pltpu.SemaphoreType.DMA(shape)

        def linked(count, width):
            return [vm(count, nr + 2, nc, width), vm(count, 2, nr, width), vm(count, 2, nr, width)]

        def linked_one(width):
            return [vm(nr + 2, nc, width), vm(1, 2, nr, width), vm(1, 2, nr, width)]

        block = (nr, nc, nz)
        flags = pltpu.VMEM((nr, flag.shape[2], nc), jnp.int32)
        scratch = [
            *linked(4, nz), *linked(3, LANES), *linked_one(nz), *linked_one(nz), *linked(4, nz), *linked(1, LANES),
            vm(7, *block), vm(6, *block), vm(*block), vm(*block), vm(*block), vm(*block), vm(*block),
            vm(3, *block), vm(*block), flags, pltpu.VMEM(look.shape, jnp.int32),
            pltpu.VMEM((nr, nc, LANES), jnp.int32), vm(nr, nc, LANES), vm(nr, nc, LANES), vm(*block),
            vm(3, nc + 16, LANES), vm(3 * nr, nc + 16, LANES), vm(3 * nr, nc + 16, LANES), vm(8, 3 * nr, nc + 16, LANES), vm(4, 3 * nr, nc + 16, LANES),
            vm(nr, LANES), vm(ny, nr, LANES), vm(2, LANES), vm(3, ny, 2, LANES),
            vm(2, nc, LANES), vm(2, 2, 1, LANES), vm(2, 2, most, 1, LANES),
            dma(9), dma(EXCHANGES, 2), dma(EXCHANGES, 2), dma(EXCHANGES, 2), dma(EXCHANGES, 2),
            dma(), dma(), dma(8), dma(8), dma(3), dma(3), dma(2, 2), dma(2, 2),
        ]
        far = pl.BlockSpec(memory_space=pltpu.HBM)
        near = pl.BlockSpec(memory_space=pltpu.VMEM)
        flag = jnp.transpose(flag, (0, 2, 1))
        return pl.pallas_call(
            functools.partial(kernel, nx, ny),
            out_shape=(jax.ShapeDtypeStruct(block, F32), jax.ShapeDtypeStruct(block, F32)),
            in_specs=[far] * 9,
            out_specs=(near, near),
            scratch_shapes=scratch,
            compiler_params=pltpu.CompilerParams(collective_id=0, has_side_effects=True, vmem_limit_bytes=40 * 1024 * 1024),
            name="window",
        )(*(pltpu.with_memory_space_constraint(a, pltpu.HBM) for a in (u, dif, vel, flag, x, cap, k, q, look)))

    spec = P("gx", "gy", None)
    return jax.shard_map(
        local,
        mesh=mesh,
        in_specs=(spec, spec, P(None, "gx", "gy", None), spec, spec, spec, spec, spec, P("gx", "gy")),
        out_specs=(spec, spec),
        check_vma=False,
    )
```

```python
import functools

import jax
import jax.numpy as jnp
from jax import lax
from jax.experimental import pallas as pl
from jax.experimental.pallas import tpu as pltpu
from jax.sharding import PartitionSpec as P

MESH = pl.DeviceIdType.MESH
SUBSTEPS = 4
LANES = 128
X_U, X_L, X_X, X_K, X_B, X_C, X_V, X_E, EXCHANGES = 0, 4, 7, 8, 9, 13, 14, 18, 19
ORDER = (
    "T", "L0", "K", "X", "LK", "CF", "G", "L1", "E", "W", "L2", "B0", "L3", "EW", "U0", "B1", "V0", "R1", "M", "B2", "C",
    "R2", "B3", "U1", "V1", "R3", "H", "U2", "V2", "A2", "U3", "V3", "A3", "U4",
)
F32 = jnp.float32


def kernel(nx, ny, u_in, dif_in, vel_in, flag_in, x_in, cap_in, k_in, q_in, look_in, u_out, x_out,
           U, HU, SU, L, HL, SL, X, HX, SX, K, HK, SK, B, HB, SB, C, HC, SC,
           CF, W, D, DI, CD, CAP, Q, VEL, DIF, FLAG, LOOK, LKC, GH, FX, DV3,
           EP, EK, EC, WE, CE, TS, TR, PS, PR, ES, ER, AW, AS, AR,
           in_sem, xs, xr, ys, yr, ts, tr, es, er, ps, pr, a_s, a_r):
    gx, gy = lax.axis_index("gx"), lax.axis_index("gy")
    nr, nc, nz = u_in.shape
    top = nz - LANES
    tiles = nz // LANES
    halves = max(1, nc * ny // LANES)
    per = LANES // nc
    waiting, leaving = {}, {}

    def turned(me, d, n):
        return me + d - jnp.where(me + d >= n, n, 0)

    def spot(mx, my):
        return {"device_id": (mx, my), "device_id_type": MESH}

    own = pl.ds(1, nr)
    loads = {}
    for name, src, dst in (
        ("x", x_in, X.at[own]), ("look", look_in, LOOK), ("u", u_in, U.at[0, own]), ("k", k_in, K.at[own]),
        ("flag", flag_in, FLAG), ("dif", dif_in, DIF), ("vel", vel_in, VEL), ("cap", cap_in, CAP), ("q", q_in, Q),
    ):
        loads[name] = pltpu.make_async_copy(src, dst, in_sem.at[len(loads)])
        loads[name].start()

    def loaded(*names):
        for name in names:
            if name in loads:
                loads.pop(name).wait()

    EP[...] = jnp.zeros_like(EP)
    ER[...] = jnp.zeros_like(ER)
    barrier = pltpu.get_barrier_semaphore()

    def greet_y(d, _):
        pl.semaphore_signal(barrier, inc=1, **spot(gx, turned(gy, d, ny)))
        return 0

    def greet_x(d, _):
        pl.semaphore_signal(barrier, inc=1, **spot(turned(gx, d, nx), gy))
        return 0

    lax.fori_loop(1, ny, greet_y, 0)
    lax.fori_loop(1, nx, greet_x, 0)
    corners = [(dx, dy) for dx in (-1, 1) for dy in (-1, 1)]

    def in_grid(dx, dy):
        return (gx + dx >= 0) & (gx + dx < nx) & (gy + dy >= 0) & (gy + dy < ny)

    for dx, dy in corners:
        @pl.when(in_grid(dx, dy))
        def _(dx=dx, dy=dy):
            pl.semaphore_signal(barrier, inc=1, **spot(lax.rem(gx + dx + nx, nx), lax.rem(gy + dy + ny, ny)))

    def all_here():
        expected = nx + ny - 2
        for dx, dy in corners:
            expected = expected + jnp.where(in_grid(dx, dy), 1, 0)
        pl.semaphore_wait(barrier, expected)

    for at_edge, row, side in ((gx == 0, 0, None), (gx == nx - 1, nr + 1, None), (gy == 0, None, 0), (gy == ny - 1, None, 1)):
        @pl.when(at_edge)
        def _(row=row, side=side):
            if side is None:
                for ext in (U, L, B, C):
                    ext[:, row] = jnp.zeros((ext.shape[0], *ext.shape[2:]), F32)
                for ext in (X, K):
                    ext[row] = jnp.zeros(ext.shape[1:], F32)
            else:
                for rim in (HU, HL, HB, HC, HX, HK):
                    rim[:, side] = jnp.zeros((rim.shape[0], *rim.shape[2:]), F32)

    up_x, dn_x, up_y, dn_y = lax.rem(gx + 1, nx), lax.rem(gx + nx - 1, nx), lax.rem(gy + 1, ny), lax.rem(gy + ny - 1, ny)

    def x_pair(ext, e):
        return (
            pltpu.make_async_remote_copy(ext.at[nr], ext.at[0], xs.at[e, 0], xr.at[e, 0], **spot(up_x, gy)),
            pltpu.make_async_remote_copy(ext.at[1], ext.at[nr + 1], xs.at[e, 1], xr.at[e, 1], **spot(dn_x, gy)),
        )

    def y_pair(stage, rim, e):
        return (
            pltpu.make_async_remote_copy(stage.at[1], rim.at[0], ys.at[e, 0], yr.at[e, 0], **spot(gx, up_y)),
            pltpu.make_async_remote_copy(stage.at[0], rim.at[1], ys.at[e, 1], yr.at[e, 1], **spot(gx, dn_y)),
        )

    def start(pair, g, n):
        @pl.when(g < n - 1)
        def _():
            pair[0].start()

        @pl.when(g > 0)
        def _():
            pair[1].start()

    def arrive(pair, g, n):
        @pl.when(g > 0)
        def _():
            pair[0].wait_recv()

        @pl.when(g < n - 1)
        def _():
            pair[1].wait_recv()

    def leave(pair, g, n):
        @pl.when(g < n - 1)
        def _():
            pair[0].wait_send()

        @pl.when(g > 0)
        def _():
            pair[1].wait_send()

    links = {}
    for k in range(4):
        links["u", k] = (U.at[k], SU.at[k], HU.at[k], X_U + k)
        links["b", k] = (B.at[k], SB.at[k], HB.at[k], X_B + k)
    for k in range(3):
        links["l", k] = (L.at[k], SL.at[k], HL.at[k], X_L + k)
    links["c", 3] = (C.at[0], SC.at[0], HC.at[0], X_C)
    links["x", 0] = (X, SX.at[0], HX.at[0], X_X)
    links["k", 0] = (K, SK.at[0], HK.at[0], X_K)

    def x_copies(name, half=0):
        ext, _, _, e = links[name]
        if name[0] != "u":
            return x_pair(ext, e)
        lanes = pl.ds(half * (nz // 2), nz // 2)
        return x_pair(ext.at[:, :, lanes], e + half * (X_V - X_U))

    def send_x(name):
        start(x_copies(name), gx, nx)

    def send_rest(k):
        pair = x_copies(("u", k), 1)
        start(pair, gx, nx)
        waiting["v", k] = lambda: arrive(pair, gx, nx)
        leaving["v", k] = lambda: leave(pair, gx, nx)

    def send_y(name):
        ext, stage, rim, e = links[name]
        start(y_pair(stage, rim, e), gy, ny)

        def came():
            arrive(y_pair(stage, rim, e), gy, ny)
            arrive(x_copies(name), gx, nx)

        def left():
            leave(y_pair(stage, rim, e), gy, ny)
            leave(x_copies(name), gx, nx)

        waiting[name], leaving[name] = came, left

    def await_halo(*names):
        for name in names:
            if name in waiting:
                waiting.pop(name)()

    def rows(body, first=0, count=None, step=1):
        def one(t, _):
            body(first + t * step)
            return 0

        lax.fori_loop(0, nr if count is None else count, one, 0)

    def put(name, i, value):
        ext, stage, _, _ = links[name]
        ext[i + 1] = value
        stage[0, pl.ds(i, 1)] = value[0:1]
        stage[1, pl.ds(i, 1)] = value[nc - 1:nc]

    def produce(name, value_of):
        rows(lambda i: put(name, i, value_of(i)), 0, 2, nr - 1)
        send_x(name)
        rows(lambda i: put(name, i, value_of(i)), 1, nr - 2)
        send_y(name)

    def stage_and_send(name):
        ext, stage, _, _ = links[name]
        send_x(name)

        def body(i):
            stage[0, pl.ds(i, 1)] = ext[i + 1, 0:1]
            stage[1, pl.ds(i, 1)] = ext[i + 1, nc - 1:nc]

        rows(body)
        send_y(name)

    def around(name, i, low=None):
        ext, _, rim, _ = links[name]
        c = ext[i + 1]
        width = c.shape[1]
        sub = lax.broadcasted_iota(jnp.int32, c.shape, 0)
        lane = lax.broadcasted_iota(jnp.int32, c.shape, 1)
        zero = jnp.zeros_like(c)
        return c, (
            ext[i],
            ext[i + 2],
            jnp.where(sub == 0, rim[0, pl.ds(i, 1)], pltpu.roll(c, 1, 0)),
            jnp.where(sub == nc - 1, rim[1, pl.ds(i, 1)], pltpu.roll(c, nc - 1, 0)),
            jnp.where(lane == 0, zero if low is None else low, pltpu.roll(c, 1, 1)),
            jnp.where(lane == width - 1, zero, pltpu.roll(c, width - 1, 1)),
        )

    def fluid(name, i):
        c, near = around(name, i, GH[i][:, 0:1])
        width = c.shape[1]
        total = CF[6, i, :, 0:width] * c
        for n in range(6):
            total = total + CF[n, i, :, 0:width] * near[n]
        return total

    def scaled_image(name, i):
        c, near = around(name, i)
        lanes = pl.ds(nz - c.shape[1], c.shape[1])
        total = CD[i, :, lanes] * c
        for n in range(6):
            total = total + W[n, i, :, lanes] * (c - near[n])
        return total

    def fluid_coefficients():
        square = (nc, nc)
        diagonal = lax.broadcasted_iota(jnp.int32, square, 0) == lax.broadcasted_iota(jnp.int32, square, 1)

        def body(i):
            flag = FLAG[i].astype(F32)
            blocks = []
            for b in range(tiles):
                column = jnp.sum(jnp.where(diagonal, jnp.broadcast_to(flag[b:b + 1], square), 0.0), axis=1, keepdims=True)
                blocks.append(jnp.broadcast_to(column, (nc, LANES)))
            on = jnp.concatenate(blocks, axis=1)
            dif = DIF[i]
            size = 6.0 * dif
            for d in range(3):
                vel = VEL[d, i]
                CF[2 * d, i] = on * (dif + jnp.maximum(vel, 0.0))
                CF[2 * d + 1, i] = on * (dif - jnp.minimum(vel, 0.0))
                size = size + jnp.abs(vel)
            CF[6, i] = 1.0 - on * size

        rows(body)

    def solid_coefficients():
        def body(i):
            c, near = around(("k", 0), i)
            cap = CAP[i]
            total = cap
            faces = [0.5 * (c + v) for v in near]
            for face in faces:
                total = total + face
            inverse = 1.0 / total
            D[i] = total
            DI[i] = inverse
            CD[i] = cap * inverse
            for n in range(6):
                W[n, i] = faces[n] * inverse

        rows(body)

    def first_scaled(i):
        c, near = around(("x", 0), i)
        total = DI[i] * Q[i]
        for n in range(6):
            total = total - W[n, i] * (c - near[n])
        return total

    def in_row(p):
        return gx, p

    def in_column(p):
        return p, gy

    def send_all(name, src_of, slots, me, n, peer_of, ssem, rsem):
        def one(d, _):
            peer = turned(me, d, n)
            pltpu.make_async_remote_copy(src_of(peer), slots.at[me], ssem, rsem, **spot(*peer_of(peer))).start()
            return 0

        lax.fori_loop(1, n, one, 0)
        most = slots.at[pl.ds(0, n - 1)]
        done = pltpu.make_async_remote_copy(most, most, ssem, rsem, **spot(*peer_of(turned(me, 1, n))))
        waiting[name], leaving[name] = done.wait_recv, done.wait_send

    sub = lax.broadcasted_iota(jnp.int32, (nc, LANES), 0)
    lane = lax.broadcasted_iota(jnp.int32, (nc, LANES), 1)
    mine = lane == lax.rem(gy, per) * nc + sub
    equal = lane == sub

    def collect_top():
        loaded("x", "look")
        for i in range(nr):
            TS[i:i + 1] = jnp.sum(jnp.where(mine, X[i + 1, :, nz - 1:nz], 0.0), axis=0, keepdims=True)
        TR[gy] = TS[...]
        all_here()
        send_all("t", lambda p: TS, TR, gy, ny, in_row, ts, tr)

    def low_start():
        loaded("u")
        rows(lambda i: put(("l", 0), i, U[0, i + 1, :, 0:LANES]))
        send_x(("l", 0))
        send_y(("l", 0))

    def partners():
        look = LOOK[...].astype(F32)
        square = (nc, nc)
        diagonal = lax.broadcasted_iota(jnp.int32, square, 0) == lax.broadcasted_iota(jnp.int32, square, 1)
        for i in range(nr):
            here = jnp.broadcast_to(look[i:i + 1], square)
            column = jnp.sum(jnp.where(diagonal, here, 0.0), axis=1, keepdims=True)
            LKC[i] = jnp.broadcast_to(column, (nc, LANES)).astype(jnp.int32)
        goal = jnp.full((nc, LANES), -1.0, F32)
        for i in range(nr):
            goal = jnp.where(lane == i * nc + sub, LKC[i].astype(F32), goal)
        PS[1:2] = jnp.max(goal, axis=0, keepdims=True)

    def ghosts():
        await_halo("t")
        for i in range(nr):
            ghost = jnp.zeros((nc, LANES), F32)
            for h in range(halves):
                line = TR[h * per, i:i + 1]
                for s in range(1, min(per, ny)):
                    line = line + TR[h * per + s, i:i + 1]
                ghost = ghost + jnp.where(LKC[i] == lane + h * LANES, line, 0.0)
            GH[i] = jnp.broadcast_to(jnp.sum(ghost, axis=1, keepdims=True), (nc, LANES))
            FX[i] = L[0, i + 1] - GH[i]

    def low_step(k):
        def value(i):
            new = fluid(("l", k), i)
            FX[i] = FX[i] + (new - GH[i])
            return new

        return value

    wide = (EP.shape[1], LANES)
    pad = (wide[0] - nc) // 2
    wide_sub = lax.broadcasted_iota(jnp.int32, wide, 0)
    wide_lane = lax.broadcasted_iota(jnp.int32, wide, 1)
    keep = LANES // 16

    def flux_home():
        await_halo(("l", 2))
        rows(low_step(2))
        value = jnp.zeros((nc, LANES), F32)
        for i in range(nr):
            value = jnp.where(lane == i * nc + sub, FX[i][:, 0:1] / SUBSTEPS, value)
        PS[0:1] = jnp.sum(value, axis=0, keepdims=True)
        PR[gy] = PS[...]
        send_all("p", lambda p: PS, PR, gy, ny, in_row, ps, pr)

    def flux_beside():
        await_halo("p")
        column = (wide_sub + (gy * nc - pad)).astype(F32)
        parts = []
        for first in range(0, ny, 4):
            total = jnp.zeros(wide, F32)
            for s in range(first, min(first + 4, ny)):
                total = jnp.where(PR[s, 1:2] == column, PR[s, 0:1], total)
            parts.append(total)
        total = functools.reduce(jnp.add, parts)
        line = jnp.zeros(wide, F32)
        for i in range(nr):
            came = jnp.sum(jnp.where((wide_lane >= i * nc) & (wide_lane < (i + 1) * nc), total, 0.0), axis=1, keepdims=True)
            line = jnp.where(wide_lane == i * wide[0] + wide_sub, came, line)
            CE[0, nr + i] = jnp.where(wide_lane == LANES - 1, WE[7, nr + i] * came, 0.0)
        ES[...] = jnp.sum(line, axis=0, keepdims=True)
        pair = (
            pltpu.make_async_remote_copy(ES, ER.at[0], xs.at[X_E, 0], xr.at[X_E, 0], **spot(up_x, gy)),
            pltpu.make_async_remote_copy(ES, ER.at[1], xs.at[X_E, 1], xr.at[X_E, 1], **spot(dn_x, gy)),
        )
        start(pair, gx, nx)
        waiting["m"] = lambda: arrive(pair, gx, nx)
        leaving["m"] = lambda: leave(pair, gx, nx)

    def edge_copies():
        loaded("k", "cap")
        total = jnp.zeros((nc, LANES), F32)
        for i in range(nr):
            at = i * 2 * keep
            total = jnp.where((lane >= at) & (lane < at + keep), pltpu.roll(K[i + 1, :, top:nz], at + keep, 1), total)
            total = jnp.where((lane >= at + keep) & (lane < at + 2 * keep), pltpu.roll(CAP[i, :, top:nz], (at + 2 * keep) % LANES, 1), total)
        EP[1, pad:pad + nc] = total
        pairs = []
        for dx in (-1, 0, 1):
            for dy in (-1, 0, 1):
                if dx or dy:
                    src = {0: pl.ds(pad, nc), 1: pl.ds(nc, pad), -1: pl.ds(pad, pad)}[dy]
                    dst = {0: pl.ds(pad, nc), 1: pl.ds(0, pad), -1: pl.ds(pad + nc, pad)}[dy]
                    target = (gx + dx >= 0) & (gx + dx < nx) & (gy + dy >= 0) & (gy + dy < ny)
                    source = (gx - dx >= 0) & (gx - dx < nx) & (gy - dy >= 0) & (gy - dy < ny)
                    to = spot(lax.rem(gx + dx + nx, nx), lax.rem(gy + dy + ny, ny))
                    n = len(pairs)
                    pairs.append((target, source, pltpu.make_async_remote_copy(EP.at[1, src], EP.at[1 - dx, dst], es.at[n], er.at[n], **to)))
        for target, _, copy in pairs:
            pl.when(target)(copy.start)

        def came():
            for _, source, copy in pairs:
                pl.when(source)(copy.wait_recv)

        def left():
            for target, _, copy in pairs:
                pl.when(target)(copy.wait_send)

        waiting["e"], leaving["e"] = came, left

    def wide_around(ref, x, count):
        c = ref[x:x + count]
        return c, (ref[x - 1:x - 1 + count], ref[x + 1:x + 1 + count], pltpu.roll(c, 1, 1), pltpu.roll(c, wide[0] - 1, 1),
                   pltpu.roll(c, 1, 2), pltpu.roll(c, LANES - 1, 2))

    def edge_coefficients():
        await_halo("e")
        for x in range(3 * nr):
            at = x % nr * 2 * keep
            packed_row = EP[x // nr]
            EK[x] = jnp.where(wide_lane >= LANES - keep, pltpu.roll(packed_row, LANES - keep - at, 1), 0.0)
            EC[x] = pltpu.roll(packed_row, LANES - 2 * keep - at, 1)

        x, count = 1, 3 * nr - 2
        block = (count, *wide)
        c, near = wide_around(EK, x, count)
        at_row = lax.broadcasted_iota(jnp.int32, block, 0) + (gx * nr - nr + x)
        across = lax.broadcasted_iota(jnp.int32, block, 1) + (gy * nc - pad)
        along = lax.broadcasted_iota(jnp.int32, block, 2)
        inside = (across >= 0) & (across < ny * nc) & (along >= LANES - keep) & (at_row >= 0) & (at_row < nx * nr)
        near = near[:5] + (jnp.where(along == LANES - 1, 0.0, near[5]),)
        faces = [0.5 * (c + v) for v in near]
        cap = EC[x:x + count]
        total = cap
        for face in faces:
            total = total + face
        inverse = jnp.where(inside, 1.0 / jnp.where(inside, total, 1.0), 0.0)
        for n in range(6):
            WE[n, x:x + count] = faces[n] * inverse
        for x_end in (0, 3 * nr - 1):
            WE[7, x_end] = jnp.zeros(wide, F32)
        WE[6, x:x + count] = jnp.where(inside, cap, 0.0) * inverse
        WE[7, x:x + count] = inverse

    def flux_arrives():
        await_halo("m")
        for side, group in ((0, 0), (1, 2)):
            for i in range(nr):
                came = jnp.sum(jnp.where(wide_lane == i * wide[0] + wide_sub, ER[side], 0.0), axis=1, keepdims=True)
                CE[0, group * nr + i] = jnp.where(wide_lane == LANES - 1, WE[7, group * nr + i] * came, 0.0)
        for k in range(1, 4):
            x, count = 1 + k, 3 * nr - 2 - 2 * k
            c, near = wide_around(CE.at[k - 1], x, count)
            total = WE[6, x:x + count] * c
            for n in range(6):
                total = total + WE[n, x:x + count] * (c - near[n])
            if k > 1:
                total = c - total
            if k > 2:
                total = 2.0 * total - CE[k - 2, x:x + count]
            CE[k, x:x + count] = total
        rows(lambda i: put(("c", 3), i, CE[3, nr + i, pad:pad + nc]))
        send_x(("c", 3))
        send_y(("c", 3))

    def field(k):
        def value(i):
            if k == 1:
                return scaled_image(("b", 0), i)
            last = B[k - 1, i + 1] - scaled_image(("b", k - 1), i)
            return last if k == 2 else 2.0 * last - B[k - 2, i + 1]

        await_halo(("b", k - 1))
        produce(("b", k), value)

    def packed(use, count):
        column = jnp.sum(AW[use], axis=1, keepdims=True)
        return jnp.sum(jnp.where(equal, column, 0.0), axis=0, keepdims=True)

    def added(slots, n):
        line = slots[0]
        for s in range(1, n):
            line = line + slots[s]
        return line

    def spread_row(use):
        line = packed(use, 0)
        AS[use, 0] = line
        AR[use, 0, gy] = line
        send_all(("row", use), lambda p: AS.at[use, 0], AR.at[use, 0], gy, ny, in_row, a_s.at[use, 0], a_r.at[use, 0])

    def spread_column(use):
        await_halo(("row", use))
        line = added(AR.at[use, 0], ny)
        AS[use, 1] = line
        AR[use, 1, gx] = line
        send_all(("column", use), lambda p: AS.at[use, 1], AR.at[use, 1], gx, nx, in_column, a_s.at[use, 1], a_r.at[use, 1])

    def collected(use):
        await_halo(("column", use))
        line = added(AR.at[use, 1], nx)
        return jnp.sum(jnp.where(equal, line, 0.0), axis=1, keepdims=True)

    zeros = jnp.zeros((nc, LANES), F32)

    def sums_of(use, first, count, body, acc=None, begin=0, end=None):
        end = tiles if end is None else end

        def one(t, acc):
            i, b = t // (end - begin), begin + lax.rem(t, end - begin)
            at = pl.ds(pl.multiple_of(b * LANES, LANES), LANES)
            return tuple(a + v for a, v in zip(acc, body(i, at)))

        return lax.fori_loop(0, nr * (end - begin), one, (zeros,) * count if acc is None else acc)

    def store_sums(use, first, acc):
        for r, a in enumerate(acc):
            AW[use, first + r:first + r + 1] = jnp.sum(a, axis=0, keepdims=True)

    def scale_sums():
        def two(i, at):
            b0 = B[0, i + 1, :, at]
            weighted = D[i, :, at] * b0
            return weighted * b0, weighted * B[1, i + 1, :, at]

        AW[0] = zeros
        store_sums(0, 0, sums_of(0, 0, 2, two))
        spread_row(0)

    kept = {}

    def most_sums():
        pair = collected(0)
        rho = jnp.where(pair[0:1] > 0.0, pair[1:2] / pair[0:1], 1.0)
        kept["rho"] = rho

        def terms(fields, i, at):
            c0, c1, c2, c3 = fields
            m1 = c1 - c2
            m2 = c2 - 0.5 * (c3 + c1)
            v1 = c1 - rho * c0
            v2 = c2 - rho * (c0 - c1)
            v3 = c3 - rho * (c0 - 2.0 * (c1 + c2))
            weight = D[i, :, at]
            w0, w1, w2, w3 = (weight * v for v in (c0, v1, v2, v3))
            DV3[i, :, at] = w3
            n1 = m1 - rho * c1
            n2 = m2 - rho * c2
            n3 = rho * (c1 - 2.0 * (m1 + m2))
            return (
                w0 * c0, w1 * c0, w2 * c0, w3 * c0,
                w0 * c1, w1 * c1, w2 * c1, w3 * c1,
                w1 * n1, w2 * n1, w3 * n1,
                w2 * n2, w3 * n2,
                -(w3 * n3),
            )

        AW[1] = zeros
        acc = sums_of(1, 0, 14, lambda i, at: terms([B[k, i + 1, :, at] for k in range(4)], i, at), None, 0, tiles - 1)
        acc = sums_of(1, 0, 14, lambda i, at: terms([B[k, i + 1, :, at] + CE[k, nr + i, pad:pad + nc] for k in range(4)], i, at),
                      acc, tiles - 1, tiles)
        store_sums(1, 0, acc)

    def last_sum():
        def last(i, acc):
            value = DV3[i] * scaled_image(("b", 3), i)
            for b in range(tiles):
                acc = acc + value[:, b * LANES:(b + 1) * LANES]
            return acc

        def last_top(i, acc):
            return acc + DV3[i, :, top:nz] * scaled_image(("c", 3), i)

        await_halo(("b", 3))
        acc = lax.fori_loop(0, nr, last, zeros)
        await_halo(("c", 3))
        acc = lax.fori_loop(0, nr, last_top, acc)
        store_sums(1, 14, (acc,))
        spread_row(1)

    def answer():
        rho = kept["rho"]
        col = collected(1)
        e = [col[r:r + 1] for r in range(15)]
        g = e[0:4]
        H = {(0, 0): e[4], (1, 0): e[5], (2, 0): e[6], (3, 0): e[7], (1, 1): e[8], (2, 1): e[9], (3, 1): e[10],
             (2, 2): e[11], (3, 2): e[12], (3, 3): e[13] + e[14]}
        inv, low = {}, {}
        for j in range(4):
            pivot = H[j, j]
            for m in range(j):
                pivot = pivot - low[j, m] * H[j, m]
            inv[j] = jnp.where(pivot > 0.0, 1.0 / pivot, 0.0)
            for i in range(j + 1, 4):
                value = H[i, j]
                for m in range(j):
                    value = value - low[j, m] * H[i, m]
                H[i, j] = value
                low[i, j] = value * inv[j]
        y = list(g)
        for i in range(4):
            for m in range(i):
                y[i] = y[i] - low[i, m] * y[m]
        y = [y[i] * inv[i] for i in range(4)]
        for i in range(3, -1, -1):
            for m in range(i + 1, 4):
                y[i] = y[i] - low[m, i] * y[m]
        f0 = y[0] - rho * (y[1] + y[2] + y[3])
        f1 = y[1] + rho * (y[2] + 2.0 * y[3])
        f2 = y[2] + 2.0 * rho * y[3]

        y[0:3] = [f0, f1, f2]

        def extra(k, i):
            return CE[k, nr + i, pad:pad + nc]

        def finish(i):
            x_out[i] = X[i + 1] + ((y[0] * B[0, i + 1] + y[1] * B[1, i + 1]) + (y[2] * B[2, i + 1] + y[3] * B[3, i + 1]))
            x_out[i, :, top:nz] = x_out[i, :, top:nz] + (
                (y[0] * extra(0, i) + y[1] * extra(1, i)) + (y[2] * extra(2, i) + y[3] * extra(3, i)))

        rows(finish)

    def coefficients():
        loaded("flag", "dif", "vel")
        fluid_coefficients()

    def solid_start():
        loaded("cap", "q")
        await_halo(("k", 0))
        solid_coefficients()

    def send_input(name, key):
        loaded(key)
        stage_and_send(name)

    def fluid_step(k):
        await_halo(("u", k - 1), ("v", k - 1))
        if k < SUBSTEPS:
            produce(("u", k), lambda i: fluid(("u", k - 1), i))
        else:
            rows(lambda i: u_out.__setitem__(i, fluid(("u", k - 1), i)))

    def low(k):
        await_halo(("l", k - 1))
        produce(("l", k), low_step(k - 1))

    def first_field():
        await_halo(("x", 0))
        produce(("b", 0), first_scaled)

    steps = {
        "T": collect_top, "L0": low_start, "LK": partners, "K": lambda: send_input(("k", 0), "k"), "X": lambda: send_input(("x", 0), "x"),
        "U0": lambda: send_input(("u", 0), "u"), "CF": coefficients, "G": ghosts, "L1": lambda: low(1), "L2": lambda: low(2),
        "L3": flux_home, "W": solid_start, "B0": first_field, "E": edge_copies, "EW": edge_coefficients, "M": flux_beside, "C": flux_arrives, "R1": scale_sums, "R2": lambda: spread_column(0),
        "R3": most_sums, "H": last_sum, "A2": lambda: spread_column(1), "A3": answer,
    }
    for k in range(1, 4):
        steps[f"B{k}"] = functools.partial(field, k)
    for k in range(1, SUBSTEPS + 1):
        steps[f"U{k}"] = functools.partial(fluid_step, k)
        steps[f"V{k - 1}"] = functools.partial(send_rest, k - 1)
    for name in ORDER:
        steps[name]()
    for left in leaving.values():
        left()


def solution(mesh):
    nx, ny = mesh.shape["gx"], mesh.shape["gy"]

    def local(u, dif, vel, flag, x, cap, k, q, look):
        nr, nc, nz = u.shape
        most = max(nx, ny)
        vm = lambda *shape: pltpu.VMEM(shape, F32)
        dma = lambda *shape: pltpu.SemaphoreType.DMA(shape)

        def linked(count, width):
            return [vm(count, nr + 2, nc, width), vm(count, 2, nr, width), vm(count, 2, nr, width)]

        def linked_one(width):
            return [vm(nr + 2, nc, width), vm(1, 2, nr, width), vm(1, 2, nr, width)]

        block = (nr, nc, nz)
        flags = pltpu.VMEM((nr, flag.shape[2], nc), jnp.int32)
        scratch = [
            *linked(4, nz), *linked(3, LANES), *linked_one(nz), *linked_one(nz), *linked(4, nz), *linked(1, LANES),
            vm(7, *block), vm(6, *block), vm(*block), vm(*block), vm(*block), vm(*block), vm(*block),
            vm(3, *block), vm(*block), flags, pltpu.VMEM(look.shape, jnp.int32),
            pltpu.VMEM((nr, nc, LANES), jnp.int32), vm(nr, nc, LANES), vm(nr, nc, LANES), vm(*block),
            vm(3, nc + 16, LANES), vm(3 * nr, nc + 16, LANES), vm(3 * nr, nc + 16, LANES), vm(8, 3 * nr, nc + 16, LANES), vm(4, 3 * nr, nc + 16, LANES),
            vm(nr, LANES), vm(ny, nr, LANES), vm(2, LANES), vm(ny, 2, LANES), vm(1, LANES), vm(2, 1, LANES),
            vm(2, nc, LANES), vm(2, 2, 1, LANES), vm(2, 2, most, 1, LANES),
            dma(9), dma(EXCHANGES, 2), dma(EXCHANGES, 2), dma(EXCHANGES, 2), dma(EXCHANGES, 2),
            dma(), dma(), dma(8), dma(8), dma(), dma(), dma(2, 2), dma(2, 2),
        ]
        far = pl.BlockSpec(memory_space=pltpu.HBM)
        near = pl.BlockSpec(memory_space=pltpu.VMEM)
        flag = jnp.transpose(flag, (0, 2, 1))
        return pl.pallas_call(
            functools.partial(kernel, nx, ny),
            out_shape=(jax.ShapeDtypeStruct(block, F32), jax.ShapeDtypeStruct(block, F32)),
            in_specs=[far] * 9,
            out_specs=(near, near),
            scratch_shapes=scratch,
            compiler_params=pltpu.CompilerParams(collective_id=0, has_side_effects=True, vmem_limit_bytes=40 * 1024 * 1024),
            name="window",
        )(*(pltpu.with_memory_space_constraint(a, pltpu.HBM) for a in (u, dif, vel, flag, x, cap, k, q, look)))

    spec = P("gx", "gy", None)
    return jax.shard_map(
        local,
        mesh=mesh,
        in_specs=(spec, spec, P(None, "gx", "gy", None), spec, spec, spec, spec, spec, P("gx", "gy")),
        out_specs=(spec, spec),
        check_vma=False,
    )
```

```python
import functools

import jax
import jax.numpy as jnp
from jax import lax
from jax.experimental import pallas as pl
from jax.experimental.pallas import tpu as pltpu
from jax.sharding import PartitionSpec as P

MESH = pl.DeviceIdType.MESH
SUBSTEPS = 4
LANES = 128
X_U, X_L, X_X, X_K, X_B, X_C, X_V, X_E, EXCHANGES = 0, 4, 7, 8, 9, 13, 14, 18, 19
ORDER = (
    "T", "L0", "K", "X", "LK", "CF", "G", "L1", "E", "W", "L2", "B0", "L3", "EW", "U0", "B1", "V0", "R1", "M", "B2", "C",
    "R2", "B3", "U1", "V1", "R3", "H", "U2", "V2", "A2", "U3", "V3", "A3", "U4",
)
F32 = jnp.float32


def kernel(nx, ny, u_in, dif_in, vel_in, flag_in, x_in, cap_in, k_in, q_in, look_in, u_out, x_out,
           U, HU, SU, L, HL, SL, X, HX, SX, K, HK, SK, B, HB, SB, C, HC, SC,
           CF, W, D, DI, CD, CAP, Q, VEL, DIF, FLAG, LOOK, LKC, GH, FX, DV3,
           EP, EK, EC, WE, CE, TS, TR, PS, PR, ES, ER, AW, AS, AR,
           in_sem, xs, xr, ys, yr, ts, tr, es, er, ps, pr, a_s, a_r):
    gx, gy = lax.axis_index("gx"), lax.axis_index("gy")
    nr, nc, nz = u_in.shape
    top = nz - LANES
    tiles = nz // LANES
    halves = max(1, nc * ny // LANES)
    per = LANES // nc
    waiting, leaving = {}, {}

    def turned(me, d, n):
        return me + d - jnp.where(me + d >= n, n, 0)

    def spot(mx, my):
        return {"device_id": (mx, my), "device_id_type": MESH}

    own = pl.ds(1, nr)
    loads = {}
    for name, src, dst in (
        ("x", x_in, X.at[own]), ("look", look_in, LOOK), ("u", u_in, U.at[0, own]), ("k", k_in, K.at[own]),
        ("flag", flag_in, FLAG), ("dif", dif_in, DIF), ("vel", vel_in, VEL), ("cap", cap_in, CAP), ("q", q_in, Q),
    ):
        loads[name] = pltpu.make_async_copy(src, dst, in_sem.at[len(loads)])
        loads[name].start()

    def loaded(*names):
        for name in names:
            if name in loads:
                loads.pop(name).wait()

    EP[...] = jnp.zeros_like(EP)
    ER[...] = jnp.zeros_like(ER)
    barrier = pltpu.get_barrier_semaphore()

    def greet_y(d, _):
        pl.semaphore_signal(barrier, inc=1, **spot(gx, turned(gy, d, ny)))
        return 0

    def greet_x(d, _):
        pl.semaphore_signal(barrier, inc=1, **spot(turned(gx, d, nx), gy))
        return 0

    lax.fori_loop(1, ny, greet_y, 0)
    lax.fori_loop(1, nx, greet_x, 0)
    greeted = [True]
    corners = [(dx, dy) for dx in (-1, 1) for dy in (-1, 1)]

    def in_grid(dx, dy):
        return (gx + dx >= 0) & (gx + dx < nx) & (gy + dy >= 0) & (gy + dy < ny)

    for dx, dy in corners:
        @pl.when(in_grid(dx, dy))
        def _(dx=dx, dy=dy):
            pl.semaphore_signal(barrier, inc=1, **spot(lax.rem(gx + dx + nx, nx), lax.rem(gy + dy + ny, ny)))

    def all_here():
        if not greeted:
            return
        greeted.clear()
        expected = nx + ny - 2
        for dx, dy in corners:
            expected = expected + jnp.where(in_grid(dx, dy), 1, 0)
        pl.semaphore_wait(barrier, expected)

    for at_edge, row, side in ((gx == 0, 0, None), (gx == nx - 1, nr + 1, None), (gy == 0, None, 0), (gy == ny - 1, None, 1)):
        @pl.when(at_edge)
        def _(row=row, side=side):
            if side is None:
                for ext in (U, L, B, C):
                    ext[:, row] = jnp.zeros((ext.shape[0], *ext.shape[2:]), F32)
                for ext in (X, K):
                    ext[row] = jnp.zeros(ext.shape[1:], F32)
            else:
                for rim in (HU, HL, HB, HC, HX, HK):
                    rim[:, side] = jnp.zeros((rim.shape[0], *rim.shape[2:]), F32)

    up_x, dn_x, up_y, dn_y = lax.rem(gx + 1, nx), lax.rem(gx + nx - 1, nx), lax.rem(gy + 1, ny), lax.rem(gy + ny - 1, ny)

    def x_pair(ext, e):
        return (
            pltpu.make_async_remote_copy(ext.at[nr], ext.at[0], xs.at[e, 0], xr.at[e, 0], **spot(up_x, gy)),
            pltpu.make_async_remote_copy(ext.at[1], ext.at[nr + 1], xs.at[e, 1], xr.at[e, 1], **spot(dn_x, gy)),
        )

    def y_pair(stage, rim, e):
        return (
            pltpu.make_async_remote_copy(stage.at[1], rim.at[0], ys.at[e, 0], yr.at[e, 0], **spot(gx, up_y)),
            pltpu.make_async_remote_copy(stage.at[0], rim.at[1], ys.at[e, 1], yr.at[e, 1], **spot(gx, dn_y)),
        )

    def start(pair, g, n):
        @pl.when(g < n - 1)
        def _():
            pair[0].start()

        @pl.when(g > 0)
        def _():
            pair[1].start()

    def arrive(pair, g, n):
        @pl.when(g > 0)
        def _():
            pair[0].wait_recv()

        @pl.when(g < n - 1)
        def _():
            pair[1].wait_recv()

    def leave(pair, g, n):
        @pl.when(g < n - 1)
        def _():
            pair[0].wait_send()

        @pl.when(g > 0)
        def _():
            pair[1].wait_send()

    links = {}
    for k in range(4):
        links["u", k] = (U.at[k], SU.at[k], HU.at[k], X_U + k)
        links["b", k] = (B.at[k], SB.at[k], HB.at[k], X_B + k)
    for k in range(3):
        links["l", k] = (L.at[k], SL.at[k], HL.at[k], X_L + k)
    links["c", 3] = (C.at[0], SC.at[0], HC.at[0], X_C)
    links["x", 0] = (X, SX.at[0], HX.at[0], X_X)
    links["k", 0] = (K, SK.at[0], HK.at[0], X_K)

    def x_copies(name, half=0):
        ext, _, _, e = links[name]
        if name[0] != "u":
            return x_pair(ext, e)
        lanes = pl.ds(half * (nz // 2), nz // 2)
        return x_pair(ext.at[:, :, lanes], e + half * (X_V - X_U))

    def send_x(name):
        start(x_copies(name), gx, nx)

    def send_rest(k):
        pair = x_copies(("u", k), 1)
        start(pair, gx, nx)
        waiting["v", k] = lambda: arrive(pair, gx, nx)
        leaving["v", k] = lambda: leave(pair, gx, nx)

    def send_y(name):
        ext, stage, rim, e = links[name]
        start(y_pair(stage, rim, e), gy, ny)

        def came():
            arrive(y_pair(stage, rim, e), gy, ny)
            arrive(x_copies(name), gx, nx)

        def left():
            leave(y_pair(stage, rim, e), gy, ny)
            leave(x_copies(name), gx, nx)

        waiting[name], leaving[name] = came, left

    def await_halo(*names):
        for name in names:
            if name in waiting:
                waiting.pop(name)()

    def rows(body, first=0, count=None, step=1):
        def one(t, _):
            body(first + t * step)
            return 0

        lax.fori_loop(0, nr if count is None else count, one, 0)

    def put(name, i, value):
        ext, stage, _, _ = links[name]
        ext[i + 1] = value
        stage[0, pl.ds(i, 1)] = value[0:1]
        stage[1, pl.ds(i, 1)] = value[nc - 1:nc]

    def produce(name, value_of):
        rows(lambda i: put(name, i, value_of(i)), 0, 2, nr - 1)
        send_x(name)
        rows(lambda i: put(name, i, value_of(i)), 1, nr - 2)
        send_y(name)

    def stage_and_send(name):
        ext, stage, _, _ = links[name]
        send_x(name)

        def body(i):
            stage[0, pl.ds(i, 1)] = ext[i + 1, 0:1]
            stage[1, pl.ds(i, 1)] = ext[i + 1, nc - 1:nc]

        rows(body)
        send_y(name)

    def around(name, i, low=None):
        ext, _, rim, _ = links[name]
        c = ext[i + 1]
        width = c.shape[1]
        sub = lax.broadcasted_iota(jnp.int32, c.shape, 0)
        lane = lax.broadcasted_iota(jnp.int32, c.shape, 1)
        zero = jnp.zeros_like(c)
        return c, (
            ext[i],
            ext[i + 2],
            jnp.where(sub == 0, rim[0, pl.ds(i, 1)], pltpu.roll(c, 1, 0)),
            jnp.where(sub == nc - 1, rim[1, pl.ds(i, 1)], pltpu.roll(c, nc - 1, 0)),
            jnp.where(lane == 0, zero if low is None else low, pltpu.roll(c, 1, 1)),
            jnp.where(lane == width - 1, zero, pltpu.roll(c, width - 1, 1)),
        )

    def fluid(name, i):
        c, near = around(name, i, GH[i][:, 0:1])
        width = c.shape[1]
        total = CF[6, i, :, 0:width] * c
        for n in range(6):
            total = total + CF[n, i, :, 0:width] * near[n]
        return total

    def scaled_image(name, i):
        c, near = around(name, i)
        lanes = pl.ds(nz - c.shape[1], c.shape[1])
        total = CD[i, :, lanes] * c
        for n in range(6):
            total = total + W[n, i, :, lanes] * (c - near[n])
        return total

    def fluid_coefficients():
        square = (nc, nc)
        diagonal = lax.broadcasted_iota(jnp.int32, square, 0) == lax.broadcasted_iota(jnp.int32, square, 1)

        def body(i):
            flag = FLAG[i].astype(F32)
            blocks = []
            for b in range(tiles):
                column = jnp.sum(jnp.where(diagonal, jnp.broadcast_to(flag[b:b + 1], square), 0.0), axis=1, keepdims=True)
                blocks.append(jnp.broadcast_to(column, (nc, LANES)))
            on = jnp.concatenate(blocks, axis=1)
            dif = DIF[i]
            size = 6.0 * dif
            for d in range(3):
                vel = VEL[d, i]
                CF[2 * d, i] = on * (dif + jnp.maximum(vel, 0.0))
                CF[2 * d + 1, i] = on * (dif - jnp.minimum(vel, 0.0))
                size = size + jnp.abs(vel)
            CF[6, i] = 1.0 - on * size

        rows(body)

    def solid_coefficients():
        def body(i):
            c, near = around(("k", 0), i)
            cap = CAP[i]
            total = cap
            faces = [0.5 * (c + v) for v in near]
            for face in faces:
                total = total + face
            inverse = 1.0 / total
            D[i] = total
            DI[i] = inverse
            CD[i] = cap * inverse
            for n in range(6):
                W[n, i] = faces[n] * inverse

        rows(body)

    def first_scaled(i):
        c, near = around(("x", 0), i)
        total = DI[i] * Q[i]
        for n in range(6):
            total = total - W[n, i] * (c - near[n])
        return total

    def in_row(p):
        return gx, p

    def in_column(p):
        return p, gy

    def send_all(name, src_of, slots, me, n, peer_of, ssem, rsem):
        def one(d, _):
            peer = turned(me, d, n)
            pltpu.make_async_remote_copy(src_of(peer), slots.at[me], ssem, rsem, **spot(*peer_of(peer))).start()
            return 0

        lax.fori_loop(1, n, one, 0, unroll=True)
        most = slots.at[pl.ds(0, n - 1)]
        done = pltpu.make_async_remote_copy(most, most, ssem, rsem, **spot(*peer_of(turned(me, 1, n))))
        waiting[name], leaving[name] = done.wait_recv, done.wait_send

    sub = lax.broadcasted_iota(jnp.int32, (nc, LANES), 0)
    lane = lax.broadcasted_iota(jnp.int32, (nc, LANES), 1)
    mine = lane == lax.rem(gy, per) * nc + sub
    equal = lane == sub

    def collect_top():
        loaded("x", "look")
        for i in range(nr):
            TS[i:i + 1] = jnp.sum(jnp.where(mine, X[i + 1, :, nz - 1:nz], 0.0), axis=0, keepdims=True)
        TR[gy] = TS[...]
        all_here()
        send_all("t", lambda p: TS, TR, gy, ny, in_row, ts, tr)

    def low_start():
        loaded("u")
        rows(lambda i: put(("l", 0), i, U[0, i + 1, :, 0:LANES]))
        all_here()
        send_x(("l", 0))
        send_y(("l", 0))

    def partners():
        look = LOOK[...].astype(F32)
        square = (nc, nc)
        diagonal = lax.broadcasted_iota(jnp.int32, square, 0) == lax.broadcasted_iota(jnp.int32, square, 1)
        for i in range(nr):
            here = jnp.broadcast_to(look[i:i + 1], square)
            column = jnp.sum(jnp.where(diagonal, here, 0.0), axis=1, keepdims=True)
            LKC[i] = jnp.broadcast_to(column, (nc, LANES)).astype(jnp.int32)
        goal = jnp.full((nc, LANES), -1.0, F32)
        for i in range(nr):
            goal = jnp.where(lane == i * nc + sub, LKC[i].astype(F32), goal)
        PS[1:2] = jnp.max(goal, axis=0, keepdims=True)

    def ghosts():
        await_halo("t")
        for i in range(nr):
            ghost = jnp.zeros((nc, LANES), F32)
            for h in range(halves):
                line = TR[h * per, i:i + 1]
                for s in range(1, min(per, ny)):
                    line = line + TR[h * per + s, i:i + 1]
                ghost = ghost + jnp.where(LKC[i] == lane + h * LANES, line, 0.0)
            GH[i] = jnp.broadcast_to(jnp.sum(ghost, axis=1, keepdims=True), (nc, LANES))
            FX[i] = L[0, i + 1] - GH[i]

    def low_step(k):
        def value(i):
            new = fluid(("l", k), i)
            FX[i] = FX[i] + (new - GH[i])
            return new

        return value

    wide = (EP.shape[1], LANES)
    pad = (wide[0] - nc) // 2
    wide_sub = lax.broadcasted_iota(jnp.int32, wide, 0)
    wide_lane = lax.broadcasted_iota(jnp.int32, wide, 1)
    keep = LANES // 16

    def flux_home():
        await_halo(("l", 2))
        rows(low_step(2))
        value = jnp.zeros((nc, LANES), F32)
        for i in range(nr):
            value = jnp.where(lane == i * nc + sub, FX[i][:, 0:1] / SUBSTEPS, value)
        PS[0:1] = jnp.sum(value, axis=0, keepdims=True)
        PR[gy] = PS[...]
        send_all("p", lambda p: PS, PR, gy, ny, in_row, ps, pr)

    def flux_beside():
        await_halo("p")
        column = (wide_sub + (gy * nc - pad)).astype(F32)
        parts = []
        for first in range(0, ny, 4):
            total = jnp.zeros(wide, F32)
            for s in range(first, min(first + 4, ny)):
                total = jnp.where(PR[s, 1:2] == column, PR[s, 0:1], total)
            parts.append(total)
        total = functools.reduce(jnp.add, parts)
        line = jnp.zeros(wide, F32)
        for i in range(nr):
            came = jnp.sum(jnp.where((wide_lane >= i * nc) & (wide_lane < (i + 1) * nc), total, 0.0), axis=1, keepdims=True)
            line = jnp.where(wide_lane == i * wide[0] + wide_sub, came, line)
            CE[0, nr + i] = jnp.where(wide_lane == LANES - 1, WE[7, nr + i] * came, 0.0)
        ES[...] = jnp.sum(line, axis=0, keepdims=True)
        pair = (
            pltpu.make_async_remote_copy(ES, ER.at[0], xs.at[X_E, 0], xr.at[X_E, 0], **spot(up_x, gy)),
            pltpu.make_async_remote_copy(ES, ER.at[1], xs.at[X_E, 1], xr.at[X_E, 1], **spot(dn_x, gy)),
        )
        start(pair, gx, nx)
        waiting["m"] = lambda: arrive(pair, gx, nx)
        leaving["m"] = lambda: leave(pair, gx, nx)

    def edge_copies():
        loaded("k", "cap")
        total = jnp.zeros((nc, LANES), F32)
        for i in range(nr):
            at = i * 2 * keep
            total = jnp.where((lane >= at) & (lane < at + keep), pltpu.roll(K[i + 1, :, top:nz], at + keep, 1), total)
            total = jnp.where((lane >= at + keep) & (lane < at + 2 * keep), pltpu.roll(CAP[i, :, top:nz], (at + 2 * keep) % LANES, 1), total)
        EP[1, pad:pad + nc] = total
        pairs = []
        for dx in (-1, 0, 1):
            for dy in (-1, 0, 1):
                if dx or dy:
                    src = {0: pl.ds(pad, nc), 1: pl.ds(nc, pad), -1: pl.ds(pad, pad)}[dy]
                    dst = {0: pl.ds(pad, nc), 1: pl.ds(0, pad), -1: pl.ds(pad + nc, pad)}[dy]
                    target = (gx + dx >= 0) & (gx + dx < nx) & (gy + dy >= 0) & (gy + dy < ny)
                    source = (gx - dx >= 0) & (gx - dx < nx) & (gy - dy >= 0) & (gy - dy < ny)
                    to = spot(lax.rem(gx + dx + nx, nx), lax.rem(gy + dy + ny, ny))
                    n = len(pairs)
                    pairs.append((target, source, pltpu.make_async_remote_copy(EP.at[1, src], EP.at[1 - dx, dst], es.at[n], er.at[n], **to)))
        for target, _, copy in pairs:
            pl.when(target)(copy.start)

        def came():
            for _, source, copy in pairs:
                pl.when(source)(copy.wait_recv)

        def left():
            for target, _, copy in pairs:
                pl.when(target)(copy.wait_send)

        waiting["e"], leaving["e"] = came, left

    def wide_around(ref, x, count):
        c = ref[x:x + count]
        return c, (ref[x - 1:x - 1 + count], ref[x + 1:x + 1 + count], pltpu.roll(c, 1, 1), pltpu.roll(c, wide[0] - 1, 1),
                   pltpu.roll(c, 1, 2), pltpu.roll(c, LANES - 1, 2))

    def edge_coefficients():
        await_halo("e")
        for x in range(3 * nr):
            at = x % nr * 2 * keep
            packed_row = EP[x // nr]
            EK[x] = jnp.where(wide_lane >= LANES - keep, pltpu.roll(packed_row, LANES - keep - at, 1), 0.0)
            EC[x] = pltpu.roll(packed_row, LANES - 2 * keep - at, 1)

        x, count = 1, 3 * nr - 2
        block = (count, *wide)
        c, near = wide_around(EK, x, count)
        at_row = lax.broadcasted_iota(jnp.int32, block, 0) + (gx * nr - nr + x)
        across = lax.broadcasted_iota(jnp.int32, block, 1) + (gy * nc - pad)
        along = lax.broadcasted_iota(jnp.int32, block, 2)
        inside = (across >= 0) & (across < ny * nc) & (along >= LANES - keep) & (at_row >= 0) & (at_row < nx * nr)
        near = near[:5] + (jnp.where(along == LANES - 1, 0.0, near[5]),)
        faces = [0.5 * (c + v) for v in near]
        cap = EC[x:x + count]
        total = cap
        for face in faces:
            total = total + face
        inverse = jnp.where(inside, 1.0 / jnp.where(inside, total, 1.0), 0.0)
        for n in range(6):
            WE[n, x:x + count] = faces[n] * inverse
        for x_end in (0, 3 * nr - 1):
            WE[7, x_end] = jnp.zeros(wide, F32)
        WE[6, x:x + count] = jnp.where(inside, cap, 0.0) * inverse
        WE[7, x:x + count] = inverse

    def flux_arrives():
        await_halo("m")
        for side, group in ((0, 0), (1, 2)):
            for i in range(nr):
                came = jnp.sum(jnp.where(wide_lane == i * wide[0] + wide_sub, ER[side], 0.0), axis=1, keepdims=True)
                CE[0, group * nr + i] = jnp.where(wide_lane == LANES - 1, WE[7, group * nr + i] * came, 0.0)
        for k in range(1, 4):
            x, count = 1 + k, 3 * nr - 2 - 2 * k
            c, near = wide_around(CE.at[k - 1], x, count)
            total = WE[6, x:x + count] * c
            for n in range(6):
                total = total + WE[n, x:x + count] * (c - near[n])
            if k > 1:
                total = c - total
            if k > 2:
                total = 2.0 * total - CE[k - 2, x:x + count]
            CE[k, x:x + count] = total
        rows(lambda i: put(("c", 3), i, CE[3, nr + i, pad:pad + nc]))
        send_x(("c", 3))
        send_y(("c", 3))

    def field(k):
        def value(i):
            if k == 1:
                return scaled_image(("b", 0), i)
            last = B[k - 1, i + 1] - scaled_image(("b", k - 1), i)
            return last if k == 2 else 2.0 * last - B[k - 2, i + 1]

        await_halo(("b", k - 1))
        produce(("b", k), value)

    def packed(use, count):
        column = jnp.sum(AW[use], axis=1, keepdims=True)
        return jnp.sum(jnp.where(equal, column, 0.0), axis=0, keepdims=True)

    def added(slots, n):
        line = slots[0]
        for s in range(1, n):
            line = line + slots[s]
        return line

    def spread_row(use):
        line = packed(use, 0)
        AS[use, 0] = line
        AR[use, 0, gy] = line
        send_all(("row", use), lambda p: AS.at[use, 0], AR.at[use, 0], gy, ny, in_row, a_s.at[use, 0], a_r.at[use, 0])

    def spread_column(use):
        await_halo(("row", use))
        line = added(AR.at[use, 0], ny)
        AS[use, 1] = line
        AR[use, 1, gx] = line
        send_all(("column", use), lambda p: AS.at[use, 1], AR.at[use, 1], gx, nx, in_column, a_s.at[use, 1], a_r.at[use, 1])

    def collected(use):
        await_halo(("column", use))
        line = added(AR.at[use, 1], nx)
        return jnp.sum(jnp.where(equal, line, 0.0), axis=1, keepdims=True)

    zeros = jnp.zeros((nc, LANES), F32)

    def sums_of(use, first, count, body, acc=None, begin=0, end=None):
        end = tiles if end is None else end

        def one(t, acc):
            i, b = t // (end - begin), begin + lax.rem(t, end - begin)
            at = pl.ds(pl.multiple_of(b * LANES, LANES), LANES)
            return tuple(a + v for a, v in zip(acc, body(i, at)))

        return lax.fori_loop(0, nr * (end - begin), one, (zeros,) * count if acc is None else acc)

    def store_sums(use, first, acc):
        for r, a in enumerate(acc):
            AW[use, first + r:first + r + 1] = jnp.sum(a, axis=0, keepdims=True)

    def scale_sums():
        def two(i, at):
            b0 = B[0, i + 1, :, at]
            weighted = D[i, :, at] * b0
            return weighted * b0, weighted * B[1, i + 1, :, at]

        AW[0] = zeros
        store_sums(0, 0, sums_of(0, 0, 2, two))
        spread_row(0)

    kept = {}

    def most_sums():
        pair = collected(0)
        rho = jnp.where(pair[0:1] > 0.0, pair[1:2] / pair[0:1], 1.0)
        kept["rho"] = rho

        def terms(fields, i, at):
            c0, c1, c2, c3 = fields
            m1 = c1 - c2
            m2 = c2 - 0.5 * (c3 + c1)
            v1 = c1 - rho * c0
            v2 = c2 - rho * (c0 - c1)
            v3 = c3 - rho * (c0 - 2.0 * (c1 + c2))
            weight = D[i, :, at]
            w0, w1, w2, w3 = (weight * v for v in (c0, v1, v2, v3))
            DV3[i, :, at] = w3
            n1 = m1 - rho * c1
            n2 = m2 - rho * c2
            n3 = rho * (c1 - 2.0 * (m1 + m2))
            return (
                w0 * c0, w1 * c0, w2 * c0, w3 * c0,
                w0 * c1, w1 * c1, w2 * c1, w3 * c1,
                w1 * n1, w2 * n1, w3 * n1,
                w2 * n2, w3 * n2,
                -(w3 * n3),
            )

        AW[1] = zeros
        acc = sums_of(1, 0, 14, lambda i, at: terms([B[k, i + 1, :, at] for k in range(4)], i, at), None, 0, tiles - 1)
        acc = sums_of(1, 0, 14, lambda i, at: terms([B[k, i + 1, :, at] + CE[k, nr + i, pad:pad + nc] for k in range(4)], i, at),
                      acc, tiles - 1, tiles)
        store_sums(1, 0, acc)

    def last_sum():
        def last(i, acc):
            value = DV3[i] * scaled_image(("b", 3), i)
            for b in range(tiles):
                acc = acc + value[:, b * LANES:(b + 1) * LANES]
            return acc

        def last_top(i, acc):
            return acc + DV3[i, :, top:nz] * scaled_image(("c", 3), i)

        name = ("b", 3)
        _, stage, rim, e = links[name]
        waiting.pop(name)
        arrive(y_pair(stage, rim, e), gy, ny)
        acc = lax.fori_loop(1, nr - 1, last, zeros)
        arrive(x_copies(name), gx, nx)
        acc = lax.fori_loop(0, 2, lambda t, total: last(t * (nr - 1), total), acc)
        await_halo(("c", 3))
        acc = lax.fori_loop(0, nr, last_top, acc)
        store_sums(1, 14, (acc,))
        spread_row(1)

    def answer():
        rho = kept["rho"]
        col = collected(1)
        e = [col[r:r + 1] for r in range(15)]
        g = e[0:4]
        H = {(0, 0): e[4], (1, 0): e[5], (2, 0): e[6], (3, 0): e[7], (1, 1): e[8], (2, 1): e[9], (3, 1): e[10],
             (2, 2): e[11], (3, 2): e[12], (3, 3): e[13] + e[14]}
        inv, low = {}, {}
        for j in range(4):
            pivot = H[j, j]
            for m in range(j):
                pivot = pivot - low[j, m] * H[j, m]
            inv[j] = jnp.where(pivot > 0.0, 1.0 / pivot, 0.0)
            for i in range(j + 1, 4):
                value = H[i, j]
                for m in range(j):
                    value = value - low[j, m] * H[i, m]
                H[i, j] = value
                low[i, j] = value * inv[j]
        y = list(g)
        for i in range(4):
            for m in range(i):
                y[i] = y[i] - low[i, m] * y[m]
        y = [y[i] * inv[i] for i in range(4)]
        for i in range(3, -1, -1):
            for m in range(i + 1, 4):
                y[i] = y[i] - low[m, i] * y[m]
        f0 = y[0] - rho * (y[1] + y[2] + y[3])
        f1 = y[1] + rho * (y[2] + 2.0 * y[3])
        f2 = y[2] + 2.0 * rho * y[3]

        y[0:3] = [f0, f1, f2]

        def extra(k, i):
            return CE[k, nr + i, pad:pad + nc]

        def finish(i):
            x_out[i] = X[i + 1] + ((y[0] * B[0, i + 1] + y[1] * B[1, i + 1]) + (y[2] * B[2, i + 1] + y[3] * B[3, i + 1]))
            x_out[i, :, top:nz] = x_out[i, :, top:nz] + (
                (y[0] * extra(0, i) + y[1] * extra(1, i)) + (y[2] * extra(2, i) + y[3] * extra(3, i)))

        rows(finish)

    def coefficients():
        loaded("flag", "dif", "vel")
        fluid_coefficients()

    def solid_start():
        loaded("cap", "q")
        await_halo(("k", 0))
        solid_coefficients()

    def send_input(name, key):
        loaded(key)
        all_here()
        stage_and_send(name)

    def fluid_step(k):
        await_halo(("u", k - 1), ("v", k - 1))
        if k < SUBSTEPS:
            produce(("u", k), lambda i: fluid(("u", k - 1), i))
        else:
            rows(lambda i: u_out.__setitem__(i, fluid(("u", k - 1), i)))

    def low(k):
        await_halo(("l", k - 1))
        produce(("l", k), low_step(k - 1))

    def first_field():
        await_halo(("x", 0))
        produce(("b", 0), first_scaled)

    steps = {
        "T": collect_top, "L0": low_start, "LK": partners, "K": lambda: send_input(("k", 0), "k"), "X": lambda: send_input(("x", 0), "x"),
        "U0": lambda: send_input(("u", 0), "u"), "CF": coefficients, "G": ghosts, "L1": lambda: low(1), "L2": lambda: low(2),
        "L3": flux_home, "W": solid_start, "B0": first_field, "E": edge_copies, "EW": edge_coefficients, "M": flux_beside, "C": flux_arrives, "R1": scale_sums, "R2": lambda: spread_column(0),
        "R3": most_sums, "H": last_sum, "A2": lambda: spread_column(1), "A3": answer,
    }
    for k in range(1, 4):
        steps[f"B{k}"] = functools.partial(field, k)
    for k in range(1, SUBSTEPS + 1):
        steps[f"U{k}"] = functools.partial(fluid_step, k)
        steps[f"V{k - 1}"] = functools.partial(send_rest, k - 1)
    for name in ORDER:
        steps[name]()
    for left in leaving.values():
        left()


def solution(mesh):
    nx, ny = mesh.shape["gx"], mesh.shape["gy"]

    def local(u, dif, vel, flag, x, cap, k, q, look):
        nr, nc, nz = u.shape
        most = max(nx, ny)
        vm = lambda *shape: pltpu.VMEM(shape, F32)
        dma = lambda *shape: pltpu.SemaphoreType.DMA(shape)

        def linked(count, width):
            return [vm(count, nr + 2, nc, width), vm(count, 2, nr, width), vm(count, 2, nr, width)]

        def linked_one(width):
            return [vm(nr + 2, nc, width), vm(1, 2, nr, width), vm(1, 2, nr, width)]

        block = (nr, nc, nz)
        flags = pltpu.VMEM((nr, flag.shape[2], nc), jnp.int32)
        scratch = [
            *linked(4, nz), *linked(3, LANES), *linked_one(nz), *linked_one(nz), *linked(4, nz), *linked(1, LANES),
            vm(7, *block), vm(6, *block), vm(*block), vm(*block), vm(*block), vm(*block), vm(*block),
            vm(3, *block), vm(*block), flags, pltpu.VMEM(look.shape, jnp.int32),
            pltpu.VMEM((nr, nc, LANES), jnp.int32), vm(nr, nc, LANES), vm(nr, nc, LANES), vm(*block),
            vm(3, nc + 16, LANES), vm(3 * nr, nc + 16, LANES), vm(3 * nr, nc + 16, LANES), vm(8, 3 * nr, nc + 16, LANES), vm(4, 3 * nr, nc + 16, LANES),
            vm(nr, LANES), vm(ny, nr, LANES), vm(2, LANES), vm(ny, 2, LANES), vm(1, LANES), vm(2, 1, LANES),
            vm(2, nc, LANES), vm(2, 2, 1, LANES), vm(2, 2, most, 1, LANES),
            dma(9), dma(EXCHANGES, 2), dma(EXCHANGES, 2), dma(EXCHANGES, 2), dma(EXCHANGES, 2),
            dma(), dma(), dma(8), dma(8), dma(), dma(), dma(2, 2), dma(2, 2),
        ]
        far = pl.BlockSpec(memory_space=pltpu.HBM)
        near = pl.BlockSpec(memory_space=pltpu.VMEM)
        flag = jnp.transpose(flag, (0, 2, 1))
        return pl.pallas_call(
            functools.partial(kernel, nx, ny),
            out_shape=(jax.ShapeDtypeStruct(block, F32), jax.ShapeDtypeStruct(block, F32)),
            in_specs=[far] * 9,
            out_specs=(near, near),
            scratch_shapes=scratch,
            compiler_params=pltpu.CompilerParams(collective_id=0, has_side_effects=True, vmem_limit_bytes=40 * 1024 * 1024),
            name="window",
        )(*(pltpu.with_memory_space_constraint(a, pltpu.HBM) for a in (u, dif, vel, flag, x, cap, k, q, look)))

    spec = P("gx", "gy", None)
    return jax.shard_map(
        local,
        mesh=mesh,
        in_specs=(spec, spec, P(None, "gx", "gy", None), spec, spec, spec, spec, spec, P("gx", "gy")),
        out_specs=(spec, spec),
        check_vma=False,
    )
```
